256 devices in a mesh: dp: 64 (over y, z, core), mp: 4 (over x).
Axes of the slice: x: 4, y: 4, z: 8, core: 2. Of those that a mesh axis runs over, the one named last changes fastest.
Arguments:
- frames: int32 [384], P('dp'), may hold values from 17 to 129, as said below
- owners: int32 [1920], P('dp'), may hold values from -1 to 63, as said below
- offsets: int32 [1920], P('dp'), may hold values from -1 to 17, as said below
- groups: int32 [384], P('dp'), may hold values from 0 to 31, as said below
- latent: bfloat16 [1920, 64, 128], P('dp'), may hold values from -12 to 12
- noise_blocks: bfloat16 [1920, 64, 128], P('dp'), may hold values from -6 to 6
- rewards: float32 [384], P('dp'), may hold values from -6 to 6
- embed_weight: bfloat16 [64, 3072], replicated, may hold values from -2 to 2
- norm_gain: float32 [3072], replicated, may hold values from 0 to 2
- mid_weight: bfloat16 [3072, 3072], P(None, 'mp'), may hold values from -1 to 1
- head_weight: bfloat16 [3072, 64], P('mp'), may hold values from -1 to 1
Outputs:
- prediction: bfloat16 [1152, 64, 128], P('dp')
- log_prob: float32 [384], P('dp')
- advantage: float32 [384], P('dp')
The draws below stay inside these ranges and needn't reach their ends.
Inputs may be any that keep to these rules, and one draw needn't show every extreme that they name: frames = 4 m + 1 for a whole m; the block counts (frames - 1) // 32 + 1 of all samples add up to exactly 1152, and some rollout device has all its samples at 129 frames. `owners`: a live slot names its owner, an empty one -1; every owner receives exactly 18 blocks; one rollout device sends at most 1 block to one owner, and in every draw some device sends that many to some owner. `offsets`: a live slot's row at its owner, rows distinct at each owner; empty slots -1. `groups`: every prompt has exactly 12 samples.
All inputs are finite; a program needn't handle non-finite values.
Results may differ from the reference program's by a relative error of at most 0.0068.
Values may be sent and summed in bfloat16 or wider, within the bound.
A program may use at most 64 MiB of HBM per device.

```python
import math
import jax
import jax.numpy as jnp
from jax import lax

D = 3072
C = 64
BT = 128
MAXB = 5
GSIZE = 12
SPD = 6
SAMPLES = 384
GROUPS = 32
OB = 18
N_DP = 64


def layout(key):
    devices = SAMPLES // SPD
    half_dev = devices // 2
    bias_key = jax.random.fold_in(key, 101)
    shift_key = jax.random.fold_in(key, 102)
    force_key = jax.random.fold_in(key, 103)
    sides_key = jax.random.fold_in(key, 104)
    frame_key = jax.random.fold_in(key, 105)
    order_key = jax.random.fold_in(key, 106)
    device_bias = jax.random.randint(bias_key, (half_dev, 1), -1, 2)
    shifts = jnp.clip(device_bias + jax.random.randint(shift_key, (half_dev, SPD), -1, 2), -2, 2)
    forced = jax.random.randint(force_key, (), 0, half_dev)
    shifts = jnp.where(jnp.arange(half_dev)[:, None] == forced, 2, shifts)
    sides = jax.random.randint(sides_key, (half_dev, 1), 0, 2)
    first_counts = jnp.where(sides == 0, 3 + shifts, 3 - shifts)
    counts = jnp.concatenate([first_counts, 6 - first_counts], axis=0)
    extra_frames = jax.random.randint(frame_key, (devices, SPD), 0, 8)
    latent_minus = jnp.where(counts == 1, jnp.maximum(extra_frames, 4), jnp.where(counts == 5, 32, 8 * (counts - 1) + extra_frames))
    frames = (4 * latent_minus + 1).reshape(-1).astype(jnp.int32)
    live_slot = (jnp.arange(MAXB)[None, None, :] < counts[:, :, None]).astype(jnp.int32)
    live_slot = live_slot.reshape(devices, SPD * MAXB)
    per_dev = jnp.sum(live_slot, axis=1)
    before = jnp.cumsum(per_dev) - per_dev
    within = jnp.cumsum(live_slot, axis=1) - 1
    global_rank = before[:, None] + within
    owner_order = jax.random.permutation(order_key, devices)
    owners = jnp.where(live_slot == 1, jnp.take(owner_order, global_rank % devices), -1)
    offsets = jnp.where(live_slot == 1, global_rank // devices, -1)
    return (frames, owners.reshape(-1).astype(jnp.int32), offsets.reshape(-1).astype(jnp.int32))


def draw_frames(key, part):
    return layout(key)[0]


def draw_owners(key, part):
    return layout(key)[1]


def draw_offsets(key, part):
    return layout(key)[2]


def draw_groups(key, part):
    return (jax.random.permutation(jax.random.fold_in(key, 7), SAMPLES) // GSIZE).astype(jnp.int32)


def base_values(key, shape, bound):
    return jnp.clip(jax.random.normal(key, shape, jnp.float32), -bound, bound)


def model_weights(key):
    embed = base_values(jax.random.fold_in(key, 201), (C, D), 6.0) / math.sqrt(C)
    gain = 1.0 + 0.15 * base_values(jax.random.fold_in(key, 202), (D,), 3.0)
    middle = base_values(jax.random.fold_in(key, 203), (D, D), 6.0) / math.sqrt(D)
    output = base_values(jax.random.fold_in(key, 204), (D, C), 6.0) / math.sqrt(D)
    return (embed, gain, middle, output)


def latent_values(key):
    raw = base_values(jax.random.fold_in(key, 205), (SAMPLES * MAXB, C, BT), 6.0)
    return raw


def rounded(values):
    narrow = lax.optimization_barrier(values.astype(jnp.bfloat16))
    return narrow.astype(jnp.float32)


def draw_latent(key, part):
    return latent_values(key).astype(jnp.bfloat16)


def draw_embed_weight(key, part):
    return model_weights(key)[0].astype(jnp.bfloat16)


def draw_norm_gain(key, part):
    return model_weights(key)[1].astype(jnp.float32)


def draw_mid_weight(key, part):
    return model_weights(key)[2].astype(jnp.bfloat16)


def draw_head_weight(key, part):
    return model_weights(key)[3].astype(jnp.bfloat16)


def draw_noise_blocks(key, part):
    embed, gain, middle, output = model_weights(key)
    embed = rounded(embed)
    middle = rounded(middle)
    output = rounded(output)
    latent = rounded(latent_values(key))

    def one_slot(block):
        embedded = jnp.dot(block.T, embed)
        mean_sq = jnp.mean(embedded * embedded, axis=-1, keepdims=True)
        normed = rounded(embedded / jnp.sqrt(mean_sq + 0.25) * gain)
        activated = rounded(jax.nn.silu(jnp.dot(normed, middle)))
        return jnp.dot(activated, output).T
    velocity = lax.map(one_slot, latent)
    sigma = jnp.exp(jax.random.uniform(jax.random.fold_in(key, 207), (SAMPLES * MAXB, 1, 1), jnp.float32, math.log(0.15), math.log(0.6)))
    fresh = base_values(jax.random.fold_in(key, 208), (SAMPLES * MAXB, C, BT), 6.0)
    return jnp.clip(sigma * fresh - velocity, -6.0, 6.0).astype(jnp.bfloat16)


def levels(rng, shape, split, least, largest):
    level, own = 1.0, jax.random.fold_in(rng, 6)
    for dim, blocks in split:
        heights = jnp.exp(jax.random.uniform(jax.random.fold_in(own, dim), (blocks,), jnp.float32, least / len(split), largest / len(split)))
        level = level * jnp.repeat(heights, shape[dim] // blocks).reshape([-1 if axis == dim else 1 for axis in range(len(shape))])
    return level


def scatter_about(stream_key, extent, spread, limit, shards=(), kind=jnp.bfloat16):
    level = levels(stream_key, extent, shards, -0.22, 0.18) if shards else 1.0
    entries = jax.random.normal(stream_key, extent, jnp.float32) * spread * level
    return jnp.minimum(jnp.maximum(entries, -limit), limit).astype(kind)


def setup_inputs(seed: int = 0) -> dict:
    key_of = jax.random.split(jax.random.key(seed), 12)
    frames = draw_frames(jax.random.fold_in(key_of[11], 71), 0)
    owners = draw_owners(jax.random.fold_in(key_of[11], 71), 0)
    offsets = draw_offsets(jax.random.fold_in(key_of[11], 71), 0)
    groups = draw_groups(jax.random.fold_in(key_of[11], 71), 0)
    latent = draw_latent(jax.random.fold_in(key_of[11], 71), 0)
    noise_blocks = draw_noise_blocks(jax.random.fold_in(key_of[11], 71), 0)
    rewards = scatter_about(key_of[6], (SAMPLES,), 1.0, 6.0, ((0, 64),), jnp.float32)
    embed_weight = draw_embed_weight(jax.random.fold_in(key_of[11], 71), 0)
    norm_gain = draw_norm_gain(jax.random.fold_in(key_of[11], 71), 0)
    mid_weight = draw_mid_weight(jax.random.fold_in(key_of[11], 71), 0)
    head_weight = draw_head_weight(jax.random.fold_in(key_of[11], 71), 0)
    return {"frames": frames, "owners": owners, "offsets": offsets, "groups": groups, "latent": latent, "noise_blocks": noise_blocks, "rewards": rewards, "embed_weight": embed_weight, "norm_gain": norm_gain, "mid_weight": mid_weight, "head_weight": head_weight}


def forward(latent_part, noise_part, embed_weight, norm_gain, mid_weight, head_weight):
    embedded = jnp.einsum('nct,cd->ntd', latent_part.astype(jnp.float32), embed_weight.astype(jnp.float32))
    mean_sq = lax.optimization_barrier(jnp.mean(embedded * embedded, axis=-1, keepdims=True))
    normed = (embedded * lax.rsqrt(mean_sq + 0.25) * norm_gain).astype(jnp.bfloat16)
    mid_out = jnp.einsum('ntd,df->ntf', normed.astype(jnp.float32), mid_weight.astype(jnp.float32))
    activated = jax.nn.silu(mid_out).astype(jnp.bfloat16)
    velocity = jnp.einsum('ntf,fc->nct', activated.astype(jnp.float32), head_weight.astype(jnp.float32))
    errors = noise_part.astype(jnp.float32) + velocity
    return (velocity.astype(jnp.bfloat16), lax.optimization_barrier(jnp.sum(errors * errors, axis=(1, 2))))

def reference(frames, owners, offsets, groups, latent, noise_blocks, rewards, embed_weight, norm_gain, mid_weight, head_weight):
    counts = ((frames - 1) // 32 + 1).astype(jnp.int32)
    slot_index = jnp.arange(SAMPLES * MAXB, dtype=jnp.int32)
    live_slot = slot_index % MAXB < jnp.repeat(counts, MAXB)
    dest_row = jnp.where(live_slot, owners * OB + offsets, N_DP * OB).astype(jnp.int32)
    owner_latent = jnp.zeros((N_DP * OB, C, BT), jnp.bfloat16).at[dest_row].set(latent, mode='drop')
    owner_noise = jnp.zeros((N_DP * OB, C, BT), jnp.bfloat16).at[dest_row].set(noise_blocks, mode='drop')
    sample_ids = (slot_index // MAXB).astype(jnp.int32)
    owner_sample = jnp.zeros((N_DP * OB,), jnp.int32).at[dest_row].set(sample_ids, mode='drop')

    def per_owner(pieces):
        return forward(pieces[0], pieces[1], embed_weight, norm_gain, mid_weight, head_weight)
    preds, slot_sums = lax.map(per_owner, (owner_latent.reshape(N_DP, OB, C, BT), owner_noise.reshape(N_DP, OB, C, BT)))
    prediction = preds.reshape(N_DP * OB, C, BT)
    totals = jax.ops.segment_sum(slot_sums.reshape(-1), owner_sample, num_segments=SAMPLES)
    log_prob = -0.5 * totals / (counts * BT * C).astype(jnp.float32)
    group_sum = jax.ops.segment_sum(rewards, groups, num_segments=GROUPS)
    group_sq = jax.ops.segment_sum(rewards * rewards, groups, num_segments=GROUPS)
    group_mean = group_sum / GSIZE
    variance = group_sq / GSIZE - group_mean * group_mean
    advantage = (rewards - group_mean[groups]) / jnp.sqrt(variance[groups] + 0.25)
    return (prediction, log_prob, advantage)
```

```python
import functools

import jax
import jax.numpy as jnp
from jax import lax
from jax.experimental import pallas as pl
from jax.experimental.pallas import tpu as pltpu
from jax.sharding import PartitionSpec as P

MESH = pl.DeviceIdType.MESH
D = 3072
C = 64
BT = 128
MAXB = 5
SPD = 6
SLOTS = 30
OB = 18
NY, NZ, NC = 4, 8, 2
NDP = NY * NZ * NC
NMP = 4
F = D // NMP
Q = C // NMP
MCH = 6
MROWS = D // MCH
CHUNKS = 3
CS = SLOTS // CHUNKS
BF = jnp.bfloat16
F32 = jnp.float32


def peer_of(k):
    me = lax.axis_index("dp")
    y, z, c = me // (NZ * NC), (me // NC) % NZ, me % NC
    a = k // (NY * NC)
    dz = NZ // 2 + (1 - 2 * (a % 2)) * ((a + 1) // 2)
    dz = jnp.where(a == NZ - 1, 0, dz)
    b = k % (NY * NC)
    dy = (2 + b // NC) % NY
    dy = jnp.where(b // NC == 2, 3, jnp.where(b // NC == 3, 0, jnp.where(b // NC == 1, 1, 2)))
    dc = 1 - b % NC
    return ((y + dy) % NY) * (NZ * NC) + ((z + dz) % NZ) * NC + (c + dc) % NC


def kernel(
    frames, owners, offsets, groups, rewards,
    gain_h, latent_h, noise_h, embed_h, mid_h, head_h,
    pred_o, logp_o, adv_o,
    ev, gv, mv, hv, lat, noi, av, lw, ht, xs, xr, predb, pay, rcv, rows,
    imeta, fmeta, itab, ftab, stab, invv, invs, idxv, idxs, ext, exr, err,
    in_sem, m_sem, loc_sem, xs_send, xs_recv, meta_send, meta_recv, a2a_send, a2a_recv,
    ag_send, ag_recv, ex_send, ex_recv,
):
    me = lax.axis_index("dp")
    j = lax.axis_index("mp")
    lane = lax.broadcasted_iota(jnp.int32, (8, 128), 1)
    sub = lax.broadcasted_iota(jnp.int32, (8, 128), 0)

    c_e = pltpu.make_async_copy(embed_h, ev, in_sem.at[0])
    c_g = pltpu.make_async_copy(gain_h, gv, in_sem.at[1])
    c_h = pltpu.make_async_copy(head_h, hv, in_sem.at[2])
    c_l = pltpu.make_async_copy(latent_h, lat, in_sem.at[3])
    c_n = pltpu.make_async_copy(noise_h.at[:, pl.ds(pl.multiple_of(j * Q, Q), Q), :], noi, in_sem.at[4])
    c_e.start()
    c_g.start()
    c_m = [
        pltpu.make_async_copy(mid_h.at[pl.ds(k * MROWS, MROWS), :], mv.at[pl.ds(k * MROWS, MROWS), :], m_sem.at[k])
        for k in range(MCH)
    ]
    for c in c_m:
        c.start()
    c_h.start()
    c_l.start()
    c_n.start()

    barrier = pltpu.get_barrier_semaphore()

    def greet(k, _):
        pl.semaphore_signal(barrier, inc=1, device_id=(peer_of(k), j), device_id_type=MESH)
        return 0

    lax.fori_loop(0, NDP - 1, greet, 0)
    for d in range(1, NMP):
        pl.semaphore_signal(barrier, inc=1, device_id=(me, (j + d) % NMP), device_id_type=MESH)

    inv = jnp.zeros((8, 128), jnp.int32)
    off = jnp.full((8, 128), -1, jnp.int32)
    counts = jnp.ones((8, 128), jnp.int32)
    for s in range(SPD):
        n = (frames[s] - 1) // 32 + 1
        counts = jnp.where(sub == s, n, counts)
        for k in range(MAXB):
            slot = s * MAXB + k
            hit = (lane == owners[slot]) & (k < n)
            inv = jnp.where(hit, slot, inv)
            off = jnp.where(hit, offsets[slot], off)
    fm = jnp.zeros((8, 128), F32)
    gown = jnp.full((8, 128), -1, jnp.int32)
    for s in range(SPD):
        off = jnp.where(lane == NDP + s, groups[s], off)
        fm = jnp.where(lane == NDP + s, rewards[s], fm)
        gown = jnp.where(sub == s, groups[s], gown)
    off = jnp.where(lane >= NDP + SPD, -2, off)
    invv[...] = inv
    imeta[...] = off[0:1, :]
    fmeta[...] = fm[0:1, :]
    c_inv = pltpu.make_async_copy(invv, invs, loc_sem.at[0])
    c_inv.start()

    c_e.wait()
    c_g.wait()
    for k in range(D // 128):
        cols = pl.ds(k * 128, 128)
        eg = ev[:, cols].astype(F32) * gv[k : k + 1, :]
        hi = eg.astype(BF)
        av[0:C, cols] = hi
        av[C : 2 * C, cols] = (eg - hi.astype(F32)).astype(BF)
    e = ev[...]
    e4 = jnp.concatenate([e, e, e, e], axis=0)
    gram = lax.dot_general(e, e4, (((1,), (1,)), ((), ())), preferred_element_type=F32)
    g1 = gram.astype(BF).astype(F32)
    g2 = (gram - g1).astype(BF).astype(F32)
    g3 = gram - g1 - g2
    gl = lax.broadcasted_iota(jnp.int32, (C, 4 * C), 1)
    gparts = jnp.where(gl < C, g1, jnp.where(gl < 2 * C, g2, jnp.where(gl < 3 * C, g3, 0.0)))
    lw[F : F + C, :] = gparts.astype(BF)
    w = jnp.zeros((2 * C, F), F32)
    for k in range(MCH):
        c_m[k].wait()
        ks = pl.ds(k * MROWS, MROWS)
        w = w + jnp.dot(av[:, ks], mv[ks, :], preferred_element_type=F32)
    w = w[0:C, :] + w[C : 2 * C, :]
    whi = w.astype(BF).astype(F32)
    wst = jnp.concatenate([whi, w - whi], axis=0)
    lw[0:F, 0 : 2 * C] = jnp.transpose(wst).astype(BF)
    lw[0:F, 2 * C : 4 * C] = jnp.zeros((F, 2 * C), BF)
    c_h.wait()
    eye = (
        lax.broadcasted_iota(jnp.int32, (C, C), 0) == lax.broadcasted_iota(jnp.int32, (C, C), 1)
    ).astype(F32).astype(BF)
    ht[...] = lax.dot_general(eye, hv[...], (((1,), (1,)), ((), ())), preferred_element_type=F32).astype(BF)
    c_l.wait()
    c_n.wait()

    pl.semaphore_wait(barrier, NDP - 1 + NMP - 1)

    def meta_copies(k):
        p = peer_of(k)
        return (
            pltpu.make_async_remote_copy(
                src_ref=imeta, dst_ref=itab.at[me], send_sem=meta_send.at[0], recv_sem=meta_recv.at[0],
                device_id=(p, j), device_id_type=MESH,
            ),
            pltpu.make_async_remote_copy(
                src_ref=fmeta, dst_ref=ftab.at[me], send_sem=meta_send.at[1], recv_sem=meta_recv.at[1],
                device_id=(p, j), device_id_type=MESH,
            ),
        )

    def send_meta(k, _):
        for c in meta_copies(k):
            c.start()
        return 0

    lax.fori_loop(0, NDP - 1, send_meta, 0)
    itab[me] = imeta[...]
    ftab[me] = fmeta[...]

    def xcopy(g, d):
        to = (j + d) % NMP
        sl = pl.ds(g * CS, CS)
        return pltpu.make_async_remote_copy(
            src_ref=xs.at[to, sl], dst_ref=xr.at[d - 1, sl],
            send_sem=xs_send.at[g, d - 1], recv_sem=xs_recv.at[g, d - 1],
            device_id=(me, to), device_id_type=MESH,
        )

    def forward(g, _):
        for p in range(CS // 2):
            s0 = g * CS + 2 * p
            x = jnp.concatenate([lat[s0], lat[s0 + 1]], axis=1)
            x4 = jnp.concatenate([x, x, x, x], axis=0)
            m = jnp.dot(lw[...], x4, preferred_element_type=F32)
            sq = jnp.sum(x.astype(F32) * m[F:, :], axis=0, keepdims=True)
            half = 0.5 * lax.rsqrt(sq * (1.0 / D) + 0.25)
            h = m[:F, :] * half
            act = (h + h * jnp.tanh(h)).astype(BF)
            vel = jnp.dot(ht[...], act, preferred_element_type=F32).astype(BF)
            for q in range(NMP):
                xs[q, s0] = vel[q * Q : (q + 1) * Q, 0:BT]
                xs[q, s0 + 1] = vel[q * Q : (q + 1) * Q, BT : 2 * BT]
        for d in (2, 1, 3):
            xcopy(g, d).start()
        return 0

    lax.fori_loop(0, CHUNKS, forward, 0)
    c_inv.wait()

    def settle(g, _):
        for d in range(1, NMP):
            xcopy(g, d).wait_recv()
        for i in range(CS // MAXB):
            s = g * (CS // MAXB) + i
            n = (frames[s] - 1) // 32 + 1
            acc = jnp.zeros((Q, BT), F32)
            for k in range(MAXB):
                slot = s * MAXB + k
                v = xs[j, slot].astype(F32) + xr[0, slot].astype(F32)
                v = v + (xr[1, slot].astype(F32) + xr[2, slot].astype(F32))
                predb[slot] = v.astype(BF)
                dlt = noi[slot].astype(F32) + v
                acc = acc + jnp.where(k < n, dlt * dlt, 0.0)
            err[s] = jnp.sum(acc, axis=0, keepdims=True)
        return 0

    lax.fori_loop(0, CHUNKS, settle, 0)

    def gather(o, _):
        pay[o] = predb[invs[0, o]]
        return 0

    lax.fori_loop(0, NDP, gather, 0)

    def block_copy(k):
        p = peer_of(k)
        return pltpu.make_async_remote_copy(
            src_ref=pay.at[p], dst_ref=rcv.at[me], send_sem=a2a_send, recv_sem=a2a_recv,
            device_id=(p, j), device_id_type=MESH,
        )

    def send_block(k, _):
        block_copy(k).start()
        return 0

    lax.fori_loop(0, NDP - 1, send_block, 0)
    rcv[me] = pay[me]

    et = jnp.zeros((8, 128), F32)
    for s in range(SPD):
        et = jnp.where(sub == s, err[s], et)
    ext[...] = et
    ex = [
        pltpu.make_async_remote_copy(
            src_ref=ext, dst_ref=exr.at[d - 1], send_sem=ex_send.at[d - 1], recv_sem=ex_recv.at[d - 1],
            device_id=(me, (j + d) % NMP), device_id_type=MESH,
        )
        for d in range(1, NMP)
    ]
    for c in ex:
        c.start()

    def all_of(ref, n, send, recv):
        return pltpu.make_async_remote_copy(
            src_ref=ref.at[pl.ds(0, n)], dst_ref=ref.at[pl.ds(0, n)], send_sem=send, recv_sem=recv,
            device_id=(me, (j + 1) % NMP), device_id_type=MESH,
        )

    all_of(itab, NDP - 1, meta_send.at[0], meta_recv.at[0]).wait_recv()
    all_of(ftab, NDP - 1, meta_send.at[1], meta_recv.at[1]).wait_recv()
    c_tab = pltpu.make_async_copy(itab, stab, loc_sem.at[1])
    c_tab.start()

    def prompt(s, carry):
        a, b = carry
        hit = gown == itab[s]
        r = jnp.where(hit & (lane >= NDP), jnp.broadcast_to(ftab[s], (8, 128)), 0.0)
        return a + r, b + r * r

    zero = jnp.zeros((8, 128), F32)
    gsum, gsq = lax.fori_loop(0, NDP, prompt, (zero, zero))
    mean = jnp.sum(gsum, axis=1, keepdims=True) * (1.0 / 12.0)
    var = jnp.sum(gsq, axis=1, keepdims=True) * (1.0 / 12.0) - mean * mean
    own = jnp.zeros((8, 128), F32)
    for s in range(SPD):
        own = jnp.where(sub == s, rewards[s], own)
    adv = (own - mean) / jnp.sqrt(var + 0.25)
    adv_o[...] = jnp.sum(jnp.where(lane == sub, adv, 0.0), axis=0, keepdims=True)

    c_tab.wait()

    def place(s, acc):
        return jnp.where(lane == stab[s, 0, me], s, acc)

    idxv[...] = lax.fori_loop(0, NDP, place, jnp.zeros((8, 128), jnp.int32))
    c_idx = pltpu.make_async_copy(idxv, idxs, loc_sem.at[2])
    c_idx.start()
    c_idx.wait()

    for c in ex:
        c.wait_recv()
    tot = jnp.sum(ext[...] + exr[0] + (exr[1] + exr[2]), axis=1, keepdims=True)
    lp = -0.5 * tot / (counts * (BT * C)).astype(F32)
    logp_o[...] = jnp.sum(jnp.where(lane == sub, lp, 0.0), axis=0, keepdims=True)

    all_of(rcv, NDP - 1, a2a_send, a2a_recv).wait_recv()

    def place_row(r, _):
        rows[r] = rcv[idxs[0, r]]
        return 0

    lax.fori_loop(0, OB, place_row, 0)
    ch = pl.ds(pl.multiple_of(j * Q, Q), Q)
    ag = [
        pltpu.make_async_remote_copy(
            src_ref=rows, dst_ref=pred_o.at[:, ch, :], send_sem=ag_send.at[d - 1], recv_sem=ag_recv.at[d - 1],
            device_id=(me, (j + d) % NMP), device_id_type=MESH,
        )
        for d in (2, 1, 3)
    ]
    for c in ag:
        c.start()
    c_own = pltpu.make_async_copy(rows, pred_o.at[:, ch, :], loc_sem.at[3])
    c_own.start()

    all_of(itab, NDP - 1, meta_send.at[0], meta_recv.at[0]).wait_send()
    all_of(ftab, NDP - 1, meta_send.at[1], meta_recv.at[1]).wait_send()
    all_of(rcv, NDP - 1, a2a_send, a2a_recv).wait_send()

    def drain(g, _):
        for d in range(1, NMP):
            xcopy(g, d).wait_send()
        return 0

    lax.fori_loop(0, CHUNKS, drain, 0)
    for c in ex:
        c.wait_send()
    c_own.wait()
    for c in ag:
        c.wait()


def local(
    frames, owners, offsets, groups, latent, noise_blocks, rewards, embed_weight, norm_gain, mid_weight, head_weight
):
    smem = pl.BlockSpec(memory_space=pltpu.SMEM)
    hbm = pl.BlockSpec(memory_space=pl.ANY)
    vmem = pl.BlockSpec(memory_space=pltpu.VMEM)
    dma = pltpu.SemaphoreType.DMA
    V = pltpu.VMEM
    scratch = [
        V((C, D), BF), V((D // 128, 128), F32), V((D, F), BF), V((F, C), BF),
        V((SLOTS, C, BT), BF), V((SLOTS, Q, BT), BF),
        V((2 * C, D), BF), V((F + C, 4 * C), BF), V((C, F), BF),
        V((NMP, SLOTS, Q, BT), BF), V((NMP - 1, SLOTS, Q, BT), BF),
        V((SLOTS, Q, BT), BF), V((NDP, Q, BT), BF), V((NDP, Q, BT), BF), V((OB, Q, BT), BF),
        V((1, 128), jnp.int32), V((1, 128), F32), V((NDP, 1, 128), jnp.int32), V((NDP, 1, 128), F32),
        pltpu.SMEM((NDP, 1, 128), jnp.int32),
        V((8, 128), jnp.int32), pltpu.SMEM((8, 128), jnp.int32),
        V((8, 128), jnp.int32), pltpu.SMEM((8, 128), jnp.int32),
        V((8, 128), F32), V((NMP - 1, 8, 128), F32), V((SPD, 1, 128), F32),
        dma((5,)), dma((MCH,)), dma((4,)),
        dma((CHUNKS, NMP - 1)), dma((CHUNKS, NMP - 1)),
        dma((2,)), dma((2,)), dma, dma,
        dma((NMP - 1,)), dma((NMP - 1,)), dma((NMP - 1,)), dma((NMP - 1,)),
    ]
    pred, logp, adv = pl.pallas_call(
        kernel,
        out_shape=(
            jax.ShapeDtypeStruct((OB, C, BT), BF),
            jax.ShapeDtypeStruct((1, 128), F32),
            jax.ShapeDtypeStruct((1, 128), F32),
        ),
        in_specs=[smem] * 5 + [hbm] * 6,
        out_specs=(hbm, vmem, vmem),
        scratch_shapes=scratch,
        compiler_params=pltpu.CompilerParams(
            collective_id=0, has_side_effects=True, vmem_limit_bytes=48 * 1024 * 1024
        ),
        name="regroup_forward",
    )(
        frames, owners, offsets, groups, rewards,
        norm_gain.reshape(D // 128, 128), latent, noise_blocks, embed_weight, mid_weight, head_weight,
    )
    return pred, logp[0, :SPD], adv[0, :SPD]


def solution(mesh):
    placed = (
        P("dp"), P("dp"), P("dp"), P("dp"), P("dp", None, None), P("dp", None, None), P("dp"),
        P(), P(), P(None, "mp"), P("mp", None),
    )
    return jax.shard_map(
        local,
        mesh=mesh,
        in_specs=placed,
        out_specs=(P("dp", None, None), P("dp"), P("dp")),
        check_vma=False,
    )
```

```python
import functools

import jax
import jax.numpy as jnp
from jax import lax
from jax.experimental import pallas as pl
from jax.experimental.pallas import tpu as pltpu
from jax.sharding import PartitionSpec as P

MESH = pl.DeviceIdType.MESH
D = 3072
C = 64
BT = 128
MAXB = 5
SPD = 6
SLOTS = 30
OB = 18
NY, NZ, NC = 4, 8, 2
NDP = NY * NZ * NC
NMP = 4
F = D // NMP
Q = C // NMP
MCH = 6
MROWS = D // MCH
CHUNKS = 3
CS = SLOTS // CHUNKS
BF = jnp.bfloat16
F32 = jnp.float32


def peer_of(k):
    return (lax.axis_index("dp") + 1 + (k + 7) % (NDP - 1)) % NDP


def kernel(
    frames_h, owners_h, offsets_h, groups_h, rewards_h,
    gain_h, latent_h, noise_h, embed_h, mid_h, head_h,
    pred_o, logp_o, adv_o,
    frames, owners, offsets, groups, rewards,
    ev, gv, mv, lat, noi, av, lw, ht, mb0, mb1, xs, xr, predb, pay, rcv, rows,
    imeta, fmeta, itab, ftab, stab, invv, invs, idxv, idxs, ext, exr, err,
    in_sem, s_sem, m_sem, loc_sem, xs_send, xs_recv, meta_send, meta_recv, a2a_send, a2a_recv,
    ag_send, ag_recv, ex_send, ex_recv,
):
    me = lax.axis_index("dp")
    j = lax.axis_index("mp")
    barrier = pltpu.get_barrier_semaphore()

    c_e = pltpu.make_async_copy(embed_h, ev, in_sem.at[0])
    c_g = pltpu.make_async_copy(gain_h, gv, in_sem.at[1])
    c_h = pltpu.make_async_copy(head_h, ht, in_sem.at[2])
    c_l = pltpu.make_async_copy(latent_h, lat, in_sem.at[3])
    c_n = pltpu.make_async_copy(noise_h.at[:, pl.ds(pl.multiple_of(j * Q, Q), Q), :], noi, in_sem.at[4])
    c_m = [
        pltpu.make_async_copy(mid_h.at[pl.ds(k * MROWS, MROWS), :], mv.at[pl.ds(k * MROWS, MROWS), :], m_sem.at[k])
        for k in range(MCH)
    ]
    c_s = [
        pltpu.make_async_copy(src, dst, s_sem.at[k])
        for k, (src, dst) in enumerate(
            ((frames_h, frames), (owners_h, owners), (offsets_h, offsets), (groups_h, groups), (rewards_h, rewards))
        )
    ]
    c_e.start()
    c_g.start()
    for c in c_m:
        c.start()
    c_l.start()
    c_h.start()
    c_n.start()
    for c in c_s:
        c.start()

    for k in range(NDP - 1):
        pl.semaphore_signal(barrier, inc=1, device_id=(peer_of(k), j), device_id_type=MESH)
    for d in range(1, NMP):
        pl.semaphore_signal(barrier, inc=1, device_id=(me, (j + d) % NMP), device_id_type=MESH)

    with jax.named_scope("prep"):
        c_e.wait()
        c_g.wait()
        for k in range(D // 128):
            cols = pl.ds(k * 128, 128)
            eg = ev[:, cols].astype(F32) * gv[k : k + 1, :]
            hi = eg.astype(BF)
            av[0:C, cols] = hi
            av[C : 2 * C, cols] = (eg - hi.astype(F32)).astype(BF)
        e = ev[...]
        e4 = jnp.concatenate([e, e, e, e], axis=0)
        gram = lax.dot_general(e, e4, (((1,), (1,)), ((), ())), preferred_element_type=F32)
        g1 = gram.astype(BF).astype(F32)
        g2 = (gram - g1).astype(BF).astype(F32)
        g3 = gram - g1 - g2
        gl = lax.broadcasted_iota(jnp.int32, (C, 4 * C), 1)
        gparts = jnp.where(gl < C, g1, jnp.where(gl < 2 * C, g2, jnp.where(gl < 3 * C, g3, 0.0)))
        lw[F : F + C, :] = gparts.astype(BF)
        w = jnp.zeros((2 * C, F), F32)
        for k in range(MCH):
            c_m[k].wait()
            ks = pl.ds(k * MROWS, MROWS)
            w = w + jnp.dot(av[:, ks], mv[ks, :], preferred_element_type=F32)
        w = w[0:C, :] + w[C : 2 * C, :]
        whi = w.astype(BF).astype(F32)
        wst = jnp.concatenate([whi, w - whi], axis=0)
        lw[0:F, 0 : 2 * C] = jnp.transpose(wst).astype(BF)
        lw[0:F, 2 * C : 4 * C] = jnp.zeros((F, 2 * C), BF)
        c_l.wait()
        c_h.wait()

    def xcopy(g, d):
        to = (j + d) % NMP
        sl = pl.ds(g * CS, CS)
        return pltpu.make_async_remote_copy(
            src_ref=xs.at[to, sl], dst_ref=xr.at[d - 1, sl],
            send_sem=xs_send.at[g, d - 1], recv_sem=xs_recv.at[g, d - 1],
            device_id=(me, to), device_id_type=MESH,
        )

    def pair(p):
        return jnp.concatenate([lat[2 * p], lat[2 * p + 1]], axis=1)

    def project(p, mb):
        x = pair(p)
        x4 = jnp.concatenate([x, x, x, x], axis=0)
        mb[...] = jnp.dot(lw[...], x4, preferred_element_type=F32)

    def finish(p, mb):
        sq = jnp.sum(pair(p).astype(F32) * mb[F:, :], axis=0, keepdims=True)
        half = 0.5 * lax.rsqrt(sq * (1.0 / D) + 0.25)
        h = mb[:F, :] * half
        act = (h + h * jnp.tanh(h)).astype(BF)
        vel = jnp.dot(ht[...], act, preferred_element_type=F32).astype(BF)
        for q in range(NMP):
            xs[q, 2 * p] = vel[q * Q : (q + 1) * Q, 0:BT]
            xs[q, 2 * p + 1] = vel[q * Q : (q + 1) * Q, BT : 2 * BT]

    mbs = (mb0, mb1)
    with jax.named_scope("forward"):
        project(0, mb0)
        for p in range(SLOTS // 2):
            if p + 1 < SLOTS // 2:
                project(p + 1, mbs[(p + 1) % 2])
            finish(p, mbs[p % 2])
            if (2 * p + 2) % CS == 0:
                if (2 * p + 2) // CS == 1:
                    pl.semaphore_wait(barrier, NDP - 1 + NMP - 1)
                for d in (2, 1, 3):
                    xcopy((2 * p + 2) // CS - 1, d).start()

    lane = lax.broadcasted_iota(jnp.int32, (8, 128), 1)
    sub = lax.broadcasted_iota(jnp.int32, (8, 128), 0)
    with jax.named_scope("meta"):
        for c in c_s:
            c.wait()
        inv = jnp.zeros((8, 128), jnp.int32)
        off = jnp.full((8, 128), -1, jnp.int32)
        counts = jnp.ones((8, 128), jnp.int32)
        fm = jnp.zeros((8, 128), F32)
        gown = jnp.full((8, 128), -1, jnp.int32)
        own = jnp.zeros((8, 128), F32)
        for s in range(SPD):
            n = (frames[s] - 1) // 32 + 1
            counts = jnp.where(sub == s, n, counts)
            for k in range(MAXB):
                slot = s * MAXB + k
                hit = (lane == owners[slot]) & (k < n)
                inv = jnp.where(hit, slot, inv)
                off = jnp.where(hit, offsets[slot], off)
            off = jnp.where(lane == NDP + s, groups[s], off)
            fm = jnp.where(lane == NDP + s, rewards[s], fm)
            gown = jnp.where(sub == s, groups[s], gown)
            own = jnp.where(sub == s, rewards[s], own)
        off = jnp.where(lane >= NDP + SPD, -2, off)
        invv[...] = inv
        imeta[...] = off[0:1, :]
        fmeta[...] = fm[0:1, :]
        itab[me] = off[0:1, :]
        ftab[me] = fm[0:1, :]
        c_inv = pltpu.make_async_copy(invv, invs, loc_sem.at[0])
        c_inv.start()

        def send_meta(k, _):
            p = peer_of(k)
            for i, (src, tab) in enumerate(((imeta, itab), (fmeta, ftab))):
                pltpu.make_async_remote_copy(
                    src_ref=src, dst_ref=tab.at[me], send_sem=meta_send.at[i], recv_sem=meta_recv.at[i],
                    device_id=(p, j), device_id_type=MESH,
                ).start()
            return 0

        lax.fori_loop(0, NDP - 1, send_meta, 0)
        c_n.wait()

    with jax.named_scope("settle"):
        for g in range(CHUNKS):
            for d in range(1, NMP):
                xcopy(g, d).wait_recv()
            for i in range(CS // MAXB):
                s = g * (CS // MAXB) + i
                n = (frames[s] - 1) // 32 + 1
                acc = jnp.zeros((Q, BT), F32)
                for k in range(MAXB):
                    slot = s * MAXB + k
                    v = xs[j, slot].astype(F32) + xr[0, slot].astype(F32)
                    v = v + (xr[1, slot].astype(F32) + xr[2, slot].astype(F32))
                    predb[slot] = v.astype(BF)
                    dlt = noi[slot].astype(F32) + v
                    acc = acc + jnp.where(k < n, dlt * dlt, 0.0)
                err[s] = jnp.sum(acc, axis=0, keepdims=True)
        c_inv.wait()

    with jax.named_scope("gather"):
        for o in range(NDP):
            pay[o] = predb[invs[0, o]]

    def send_block(k, _):
        p = peer_of(k)
        pltpu.make_async_remote_copy(
            src_ref=pay.at[p], dst_ref=rcv.at[me], send_sem=a2a_send, recv_sem=a2a_recv,
            device_id=(p, j), device_id_type=MESH,
        ).start()
        return 0

    with jax.named_scope("send_block"):
        lax.fori_loop(0, NDP - 1, send_block, 0)
        rcv[me] = pay[me]

    et = jnp.zeros((8, 128), F32)
    for s in range(SPD):
        et = jnp.where(sub == s, err[s], et)
    ext[...] = et
    ex = [
        pltpu.make_async_remote_copy(
            src_ref=ext, dst_ref=exr.at[d - 1], send_sem=ex_send.at[d - 1], recv_sem=ex_recv.at[d - 1],
            device_id=(me, (j + d) % NMP), device_id_type=MESH,
        )
        for d in range(1, NMP)
    ]
    for c in ex:
        c.start()

    def all_of(ref, n, send, recv):
        return pltpu.make_async_remote_copy(
            src_ref=ref.at[pl.ds(0, n)], dst_ref=ref.at[pl.ds(0, n)], send_sem=send, recv_sem=recv,
            device_id=(me, (j + 1) % NMP), device_id_type=MESH,
        )

    with jax.named_scope("tables"):
        all_of(itab, NDP - 1, meta_send.at[0], meta_recv.at[0]).wait_recv()
        all_of(ftab, NDP - 1, meta_send.at[1], meta_recv.at[1]).wait_recv()
        c_tab = pltpu.make_async_copy(itab, stab, loc_sem.at[1])
        c_tab.start()

        def prompt(s, carry):
            a, b = carry
            hit = gown == itab[s]
            r = jnp.where(hit & (lane >= NDP), jnp.broadcast_to(ftab[s], (8, 128)), 0.0)
            return a + r, b + r * r

        zero = jnp.zeros((8, 128), F32)
        gsum, gsq = lax.fori_loop(0, NDP, prompt, (zero, zero))
        mean = jnp.sum(gsum, axis=1, keepdims=True) * (1.0 / 12.0)
        var = jnp.sum(gsq, axis=1, keepdims=True) * (1.0 / 12.0) - mean * mean
        adv = (own - mean) / jnp.sqrt(var + 0.25)
        adv_o[...] = jnp.sum(jnp.where(lane == sub, adv, 0.0), axis=0, keepdims=True)
        c_tab.wait()
        idx = jnp.zeros((8, 128), jnp.int32)
        for s in range(NDP):
            idx = jnp.where(lane == stab[s, 0, me], s, idx)
        idxv[...] = idx
        c_idx = pltpu.make_async_copy(idxv, idxs, loc_sem.at[2])
        c_idx.start()
        c_idx.wait()
        for c in ex:
            c.wait_recv()
        tot = jnp.sum(ext[...] + exr[0] + (exr[1] + exr[2]), axis=1, keepdims=True)
        lp = -0.5 * tot / (counts * (BT * C)).astype(F32)
        logp_o[...] = jnp.sum(jnp.where(lane == sub, lp, 0.0), axis=0, keepdims=True)

    with jax.named_scope("a2a_wait"):
        all_of(rcv, NDP - 1, a2a_send, a2a_recv).wait_recv()
    for r in range(OB):
        rows[r] = rcv[idxs[0, r]]
    ch = pl.ds(pl.multiple_of(j * Q, Q), Q)
    ag = [
        pltpu.make_async_remote_copy(
            src_ref=rows, dst_ref=pred_o.at[:, ch, :], send_sem=ag_send.at[d - 1], recv_sem=ag_recv.at[d - 1],
            device_id=(me, (j + d) % NMP), device_id_type=MESH,
        )
        for d in (2, 1, 3)
    ]
    for c in ag:
        c.start()
    c_own = pltpu.make_async_copy(rows, pred_o.at[:, ch, :], loc_sem.at[3])
    c_own.start()

    with jax.named_scope("final_wait"):
        all_of(itab, NDP - 1, meta_send.at[0], meta_recv.at[0]).wait_send()
        all_of(ftab, NDP - 1, meta_send.at[1], meta_recv.at[1]).wait_send()
        all_of(rcv, NDP - 1, a2a_send, a2a_recv).wait_send()
        for g in range(CHUNKS):
            for d in range(1, NMP):
                xcopy(g, d).wait_send()
        for c in ex:
            c.wait_send()
        c_own.wait()
        for c in ag:
            c.wait()


def local(
    frames, owners, offsets, groups, latent, noise_blocks, rewards, embed_weight, norm_gain, mid_weight, head_weight
):
    hbm = pl.BlockSpec(memory_space=pl.ANY)
    vmem = pl.BlockSpec(memory_space=pltpu.VMEM)
    dma = pltpu.SemaphoreType.DMA
    V = pltpu.VMEM
    S = pltpu.SMEM
    scratch = [
        S((SPD,), jnp.int32), S((SLOTS,), jnp.int32), S((SLOTS,), jnp.int32), S((SPD,), jnp.int32), S((SPD,), F32),
        V((C, D), BF), V((D // 128, 128), F32), V((D, F), BF),
        V((SLOTS, C, BT), BF), V((SLOTS, Q, BT), BF),
        V((2 * C, D), BF), V((F + C, 4 * C), BF), V((C, F), BF), V((F + C, 2 * BT), F32), V((F + C, 2 * BT), F32),
        V((NMP, SLOTS, Q, BT), BF), V((NMP - 1, SLOTS, Q, BT), BF),
        V((SLOTS, Q, BT), BF), V((NDP, Q, BT), BF), V((NDP, Q, BT), BF), V((OB, Q, BT), BF),
        V((1, 128), jnp.int32), V((1, 128), F32), V((NDP, 1, 128), jnp.int32), V((NDP, 1, 128), F32),
        pltpu.SMEM((NDP, 1, 128), jnp.int32),
        V((8, 128), jnp.int32), pltpu.SMEM((8, 128), jnp.int32),
        V((8, 128), jnp.int32), pltpu.SMEM((8, 128), jnp.int32),
        V((8, 128), F32), V((NMP - 1, 8, 128), F32), V((SPD, 1, 128), F32),
        dma((5,)), dma((5,)), dma((MCH,)), dma((4,)),
        dma((CHUNKS, NMP - 1)), dma((CHUNKS, NMP - 1)),
        dma((2,)), dma((2,)), dma, dma,
        dma((NMP - 1,)), dma((NMP - 1,)), dma((NMP - 1,)), dma((NMP - 1,)),
    ]
    pred, logp, adv = pl.pallas_call(
        kernel,
        out_shape=(
            jax.ShapeDtypeStruct((OB, C, BT), BF),
            jax.ShapeDtypeStruct((1, 128), F32),
            jax.ShapeDtypeStruct((1, 128), F32),
        ),
        in_specs=[hbm] * 11,
        out_specs=(hbm, vmem, vmem),
        scratch_shapes=scratch,
        compiler_params=pltpu.CompilerParams(
            collective_id=0, has_side_effects=True, vmem_limit_bytes=67043328
        ),
        name="regroup_forward",
    )(
        frames, owners, offsets, groups, rewards,
        norm_gain.reshape(D // 128, 128), latent, noise_blocks, embed_weight, mid_weight, head_weight.T,
    )
    return pred, logp[0, :SPD], adv[0, :SPD]


def solution(mesh):
    placed = (
        P("dp"), P("dp"), P("dp"), P("dp"), P("dp", None, None), P("dp", None, None), P("dp"),
        P(), P(), P(None, "mp"), P("mp", None),
    )
    return jax.shard_map(
        local,
        mesh=mesh,
        in_specs=placed,
        out_specs=(P("dp", None, None), P("dp"), P("dp")),
        check_vma=False,
    )
```

```python
import functools

import jax
import jax.numpy as jnp
from jax import lax
from jax.experimental import pallas as pl
from jax.experimental.pallas import tpu as pltpu
from jax.sharding import PartitionSpec as P

MESH = pl.DeviceIdType.MESH
D = 3072
C = 64
BT = 128
MAXB = 5
SPD = 6
SLOTS = 30
OB = 18
NY, NZ, NC = 4, 8, 2
NDP = NY * NZ * NC
NMP = 4
F = D // NMP
Q = C // NMP
HQ = Q // 2
MCH = 4
MROWS = D // MCH
RB = 128
CHUNKS = 6
CS = SLOTS // CHUNKS
OPEN = 3
SENDS = {
    1: (), 2: (), 3: ((0, 0, 3),), 4: ((0, 3, 1),), 5: ((0, 4, 1),), 6: ((0, 5, 1), (1, 0, 3), (1, 3, 3)),
}
SHARES = tuple(sorted(s for sends in SENDS.values() for s in sends))
BF = jnp.bfloat16
F32 = jnp.float32


def far(k):
    z, y = (k // NC) % NZ, k // (NC * NZ)
    return min(z, NZ - z) + min(y, NY - y)


SHIFTS = sorted(range(1, NDP), key=far, reverse=True)


def peer_of(k):
    return lax.rem(lax.axis_index("dp") + k, NDP)


def kernel(
    frames_h, owners_h, offsets_h, groups_h, rewards_h,
    gain_h, latent_h, noise_h, embed_h, mid_h, head_h,
    pred_o, logp_o, adv_o,
    frames, owners, offsets, groups, rewards,
    ev, gv, mv, lat, noi, av, lw, ht, hb, act0, act1, xs, xr, predb, pay, rcv0, rcv1, rows,
    izt, fzt, itab, ftab, stab, invv, invs, idxv, idxs, ext, exr, err,
    in_sem, s_sem, m_sem, loc_sem, xs_send, xs_recv, z_send, z_recv, meta_send, meta_recv, a2a_send, a2a_recv,
    ag_send, ag_recv, ex_send, ex_recv,
):
    me = lax.axis_index("dp")
    j = lax.axis_index("mp")
    barrier = pltpu.get_barrier_semaphore()

    c_e = pltpu.make_async_copy(embed_h, ev, in_sem.at[0])
    c_g = pltpu.make_async_copy(gain_h, gv, in_sem.at[1])
    c_h = pltpu.make_async_copy(head_h, ht, in_sem.at[2])
    c_l = pltpu.make_async_copy(latent_h, lat, in_sem.at[3])
    c_n = pltpu.make_async_copy(noise_h.at[:, pl.ds(pl.multiple_of(j * Q, Q), Q), :], noi, in_sem.at[4])
    c_m = [
        pltpu.make_async_copy(mid_h.at[pl.ds(k * MROWS, MROWS), :], mv.at[pl.ds(k * MROWS, MROWS), :], m_sem.at[k])
        for k in range(MCH)
    ]
    c_s = [
        pltpu.make_async_copy(src, dst, s_sem.at[k])
        for k, (src, dst) in enumerate(
            ((frames_h, frames), (owners_h, owners), (offsets_h, offsets), (groups_h, groups), (rewards_h, rewards))
        )
    ]
    c_e.start()
    c_g.start()
    c_l.start()
    for c in c_m:
        c.start()
    for c in c_s:
        c.start()

    for k in SHIFTS:
        pl.semaphore_signal(barrier, inc=1, device_id=(peer_of(k), j), device_id_type=MESH)
    for d in range(1, NMP):
        pl.semaphore_signal(barrier, inc=1, device_id=(me, (j + d) % NMP), device_id_type=MESH)

    c_h.start()
    c_n.start()

    lane = lax.broadcasted_iota(jnp.int32, (8, 128), 1)
    sub = lax.broadcasted_iota(jnp.int32, (8, 128), 0)
    zi = (me // NC) % NZ
    yc = (me // (NZ * NC)) * NC + me % NC
    with jax.named_scope("index"):
        for c in c_s:
            c.wait()
        inv = jnp.zeros((8, 128), jnp.int32)
        off = jnp.full((8, 128), -1, jnp.int32)
        counts = jnp.ones((8, 128), jnp.int32)
        fm = jnp.zeros((8, 128), F32)
        gown = jnp.full((8, 128), -1, jnp.int32)
        own = jnp.zeros((8, 128), F32)
        for s in range(SPD):
            n = (frames[s] - 1) // 32 + 1
            counts = jnp.where(sub == s, n, counts)
            for k in range(MAXB):
                slot = s * MAXB + k
                hit = (lane == owners[slot]) & (k < n)
                inv = jnp.where(hit, slot, inv)
                off = jnp.where(hit, offsets[slot], off)
            off = jnp.where(lane == NDP + s, groups[s], off)
            fm = jnp.where(lane == NDP + s, rewards[s], fm)
            gown = jnp.where(sub == s, groups[s], gown)
            own = jnp.where(sub == s, rewards[s], own)
        off = jnp.where(lane >= NDP + SPD, -2, off)
        invv[...] = inv
        izt[zi] = off[0:1, :]
        fzt[zi] = fm[0:1, :]
        c_inv = pltpu.make_async_copy(invv, invs, loc_sem.at[0])
        c_inv.start()

    def pair(p):
        return jnp.concatenate([lat[2 * p], lat[2 * p + 1]], axis=1)

    def stack(x):
        return jnp.concatenate([x, x, x, x], axis=0)

    with jax.named_scope("norm"):
        c_e.wait()
        c_g.wait()
        for k in range(D // 128):
            cols = pl.ds(k * 128, 128)
            eg = ev[:, cols].astype(F32) * gv[k : k + 1, :]
            hi = eg.astype(BF)
            av[0:C, cols] = hi
            av[C : 2 * C, cols] = (eg - hi.astype(F32)).astype(BF)
        gram = jnp.zeros((C, 2 * C), F32)
        for k in range(2):
            e = ev[:, pl.ds(k * (D // 2), D // 2)]
            gram = gram + lax.dot_general(
                e, jnp.concatenate([e, e], axis=0), (((1,), (1,)), ((), ())), preferred_element_type=F32
            )
        g1 = gram.astype(BF).astype(F32)
        g2 = (gram - g1).astype(BF).astype(F32)
        g3 = gram - g1 - g2
        gl = lax.broadcasted_iota(jnp.int32, (C, 2 * C), 1)
        gparts = jnp.concatenate([jnp.where(gl < C, g1, g2), jnp.where(gl < C, g3, 0.0)], axis=1).astype(BF)
        c_l.wait()
        for p in range(SLOTS // 2):
            x = pair(p)
            gx = jnp.dot(gparts, stack(x), preferred_element_type=F32)
            sq = jnp.sum(x.astype(F32) * gx, axis=0, keepdims=True)
            hb[p] = 0.5 * lax.rsqrt(sq * (1.0 / D) + 0.25)

    with jax.named_scope("fold"):
        w = jnp.zeros((2 * C, F), F32)
        for k in range(MCH):
            c_m[k].wait()
            ks = pl.ds(k * MROWS, MROWS)
            w = w + jnp.dot(av[:, ks], mv[ks, :], preferred_element_type=F32)
        w = w[0:C, :] + w[C : 2 * C, :]
        whi = w.astype(BF).astype(F32)
        wst = jnp.concatenate([whi, w - whi], axis=0)
        lw[:, 0 : 2 * C] = jnp.transpose(wst).astype(BF)
        lw[:, 2 * C : 4 * C] = jnp.zeros((F, 2 * C), BF)
        c_h.wait()

    def xcopy(h, g, n, d):
        to = (j + d) % NMP
        sl = pl.ds(g * CS, n * CS)
        return pltpu.make_async_remote_copy(
            src_ref=xs.at[h, to, sl], dst_ref=xr.at[h, d - 1, sl],
            send_sem=xs_send.at[h, g, d - 1], recv_sem=xs_recv.at[h, g, d - 1],
            device_id=(me, to), device_id_type=MESH,
        )

    def z_copies(k):
        to = (me // (NZ * NC)) * (NZ * NC) + lax.rem(zi + k, NZ) * NC + me % NC
        return [
            pltpu.make_async_remote_copy(
                src_ref=t.at[zi], dst_ref=t.at[zi], send_sem=z_send.at[i], recv_sem=z_recv.at[i],
                device_id=(to, j), device_id_type=MESH,
            )
            for i, t in enumerate((izt, fzt))
        ]

    def yc_copies(k):
        q = lax.rem(yc + k, NY * NC)
        to = (q // NC) * (NZ * NC) + zi * NC + q % NC
        return [
            pltpu.make_async_remote_copy(
                src_ref=t, dst_ref=tab.at[pl.ds(yc * NZ, NZ)], send_sem=meta_send.at[i], recv_sem=meta_recv.at[i],
                device_id=(to, j), device_id_type=MESH,
            )
            for i, (t, tab) in enumerate(((izt, itab), (fzt, ftab)))
        ]

    def all_of(ref, n, send, recv):
        return pltpu.make_async_remote_copy(
            src_ref=ref.at[pl.ds(0, n)], dst_ref=ref.at[pl.ds(0, n)], send_sem=send, recv_sem=recv,
            device_id=(me, (j + 1) % NMP), device_id_type=MESH,
        )

    acts = (act0, act1)
    rcvs = (rcv0, rcv1)

    def hidden(p, act):
        x4 = stack(pair(p))
        half = hb[p]
        for b in range(F // RB):
            rs = pl.ds(b * RB, RB)
            h = jnp.dot(lw[rs, :], x4, preferred_element_type=F32) * half
            act[rs, :] = (h + h * jnp.tanh(h)).astype(BF)

    def head(p, act):
        vel = jnp.dot(ht[...], act[...], preferred_element_type=F32).astype(BF)
        for q in range(NMP):
            for h in range(2):
                rs = slice(q * Q + h * HQ, q * Q + (h + 1) * HQ)
                xs[h, q, 2 * p] = vel[rs, 0:BT]
                xs[h, q, 2 * p + 1] = vel[rs, BT : 2 * BT]

    with jax.named_scope("forward"):
        done = 0
        hidden(0, act0)
        for p in range(SLOTS // 2):
            if p + 1 < SLOTS // 2:
                hidden(p + 1, acts[(p + 1) % 2])
            head(p, acts[p % 2])
            while (done + 1) * CS <= 2 * p + 2:
                done += 1
                if done == OPEN:
                    pl.semaphore_wait(barrier, NDP - 1 + NMP - 1)
                    for k in range(1, NZ):
                        for c in z_copies(k):
                            c.start()
                for h, g, n in SENDS[done]:
                    for d in (2, 1, 3):
                        xcopy(h, g, n, d).start()

    with jax.named_scope("meta"):
        all_of(izt, NZ - 1, z_send.at[0], z_recv.at[0]).wait_recv()
        all_of(fzt, NZ - 1, z_send.at[1], z_recv.at[1]).wait_recv()
        for k in range(1, NY * NC):
            for c in yc_copies(k):
                c.start()
        itab[pl.ds(yc * NZ, NZ)] = izt[...]
        ftab[pl.ds(yc * NZ, NZ)] = fzt[...]
        c_n.wait()

    def settle(h):
        for share in SHARES:
            if share[0] != h:
                continue
            for d in range(1, NMP):
                xcopy(*share, d).wait_recv()
            for s in range(share[1], share[1] + share[2]):
                n = (frames[s] - 1) // 32 + 1
                acc = jnp.zeros((HQ, BT), F32)
                for k in range(MAXB):
                    slot = s * MAXB + k
                    v = xs[h, j, slot].astype(F32) + xr[h, 0, slot].astype(F32)
                    v = v + (xr[h, 1, slot].astype(F32) + xr[h, 2, slot].astype(F32))
                    predb[h, slot] = v.astype(BF)
                    dlt = noi[slot, h * HQ : (h + 1) * HQ, :].astype(F32) + v
                    acc = acc + jnp.where(k < n, dlt * dlt, 0.0)
                err[h, s] = jnp.sum(acc, axis=0, keepdims=True)

    def send_blocks(h):
        for o in range(NDP):
            pay[h, o] = predb[h, invs[0, o]]
        for k in SHIFTS:
            p = peer_of(k)
            pltpu.make_async_remote_copy(
                src_ref=pay.at[h, p], dst_ref=rcvs[h].at[me], send_sem=a2a_send.at[h], recv_sem=a2a_recv.at[h],
                device_id=(p, j), device_id_type=MESH,
            ).start()
        rcvs[h][me] = pay[h, me]

    for h in range(2):
        with jax.named_scope("settle%d" % h):
            settle(h)
            if h == 0:
                c_inv.wait()
        with jax.named_scope("send_block%d" % h):
            send_blocks(h)

    et = jnp.zeros((8, 128), F32)
    for s in range(SPD):
        et = jnp.where(sub == s, err[0, s] + err[1, s], et)
    ext[...] = et
    ex = [
        pltpu.make_async_remote_copy(
            src_ref=ext, dst_ref=exr.at[d - 1], send_sem=ex_send.at[d - 1], recv_sem=ex_recv.at[d - 1],
            device_id=(me, (j + d) % NMP), device_id_type=MESH,
        )
        for d in range(1, NMP)
    ]
    for c in ex:
        c.start()

    with jax.named_scope("tables"):
        all_of(itab, NDP - NZ, meta_send.at[0], meta_recv.at[0]).wait_recv()
        all_of(ftab, NDP - NZ, meta_send.at[1], meta_recv.at[1]).wait_recv()
        c_tab = pltpu.make_async_copy(itab, stab, loc_sem.at[1])
        c_tab.start()

        def prompt(s, carry):
            a, b = carry
            hit = gown == itab[s]
            r = jnp.where(hit & (lane >= NDP), jnp.broadcast_to(ftab[s], (8, 128)), 0.0)
            return a + r, b + r * r

        zero = jnp.zeros((8, 128), F32)
        gsum, gsq = lax.fori_loop(0, NDP, prompt, (zero, zero))
        mean = jnp.sum(gsum, axis=1, keepdims=True) * (1.0 / 12.0)
        var = jnp.sum(gsq, axis=1, keepdims=True) * (1.0 / 12.0) - mean * mean
        adv = (own - mean) / jnp.sqrt(var + 0.25)
        adv_o[...] = jnp.sum(jnp.where(lane == sub, adv, 0.0), axis=0, keepdims=True)
        c_tab.wait()
        idx = jnp.zeros((8, 128), jnp.int32)
        for s in range(NDP):
            src = (s // NZ // NC) * (NZ * NC) + (s % NZ) * NC + (s // NZ) % NC
            idx = jnp.where(lane == stab[s, 0, me], src, idx)
        idxv[...] = idx
        c_idx = pltpu.make_async_copy(idxv, idxs, loc_sem.at[2])
        c_idx.start()
        c_idx.wait()

    def gather_copy(h, d):
        return pltpu.make_async_remote_copy(
            src_ref=rows.at[h], dst_ref=pred_o.at[:, pl.ds(pl.multiple_of(j * Q + h * HQ, HQ), HQ), :],
            send_sem=ag_send.at[h, d - 1], recv_sem=ag_recv.at[h, d - 1],
            device_id=(me, (j + d) % NMP), device_id_type=MESH,
        )

    for h in range(2):
        with jax.named_scope("a2a_wait%d" % h):
            all_of(rcvs[h], NDP - 1, a2a_send.at[h], a2a_recv.at[h]).wait_recv()
        for r in range(OB):
            block = rcvs[h][idxs[0, r]]
            rows[h, r] = block
            pred_o[r, pl.ds(pl.multiple_of(j * Q + h * HQ, HQ), HQ), :] = block
        for d in (2, 1, 3):
            gather_copy(h, d).start()
        if h == 0:
            for c in ex:
                c.wait_recv()
            tot = jnp.sum(ext[...] + exr[0] + (exr[1] + exr[2]), axis=1, keepdims=True)
            lp = -0.5 * tot / (counts * (BT * C)).astype(F32)
            logp_o[...] = jnp.sum(jnp.where(lane == sub, lp, 0.0), axis=0, keepdims=True)

    with jax.named_scope("final_wait"):
        all_of(izt, NZ - 1, z_send.at[0], z_recv.at[0]).wait_send()
        all_of(fzt, NZ - 1, z_send.at[1], z_recv.at[1]).wait_send()
        all_of(itab, NDP - NZ, meta_send.at[0], meta_recv.at[0]).wait_send()
        all_of(ftab, NDP - NZ, meta_send.at[1], meta_recv.at[1]).wait_send()
        for share in SHARES:
            for d in range(1, NMP):
                xcopy(*share, d).wait_send()
        for c in ex:
            c.wait_send()
        for h in range(2):
            all_of(rcvs[h], NDP - 1, a2a_send.at[h], a2a_recv.at[h]).wait_send()
            for d in range(1, NMP):
                gather_copy(h, d).wait()


def local(
    frames, owners, offsets, groups, latent, noise_blocks, rewards, embed_weight, norm_gain, mid_weight, head_weight
):
    hbm = pl.BlockSpec(memory_space=pl.ANY)
    vmem = pl.BlockSpec(memory_space=pltpu.VMEM)
    dma = pltpu.SemaphoreType.DMA
    V = pltpu.VMEM
    S = pltpu.SMEM
    scratch = [
        S((SPD,), jnp.int32), S((SLOTS,), jnp.int32), S((SLOTS,), jnp.int32), S((SPD,), jnp.int32), S((SPD,), F32),
        V((C, D), BF), V((D // 128, 128), F32), V((D, F), BF),
        V((SLOTS, C, BT), BF), V((SLOTS, Q, BT), BF),
        V((2 * C, D), BF), V((F, 4 * C), BF), V((C, F), BF),
        V((SLOTS // 2, 1, 2 * BT), F32), V((F, 2 * BT), BF), V((F, 2 * BT), BF),
        V((2, NMP, SLOTS, HQ, BT), BF), V((2, NMP - 1, SLOTS, HQ, BT), BF),
        V((2, SLOTS, HQ, BT), BF), V((2, NDP, HQ, BT), BF), V((NDP, HQ, BT), BF), V((NDP, HQ, BT), BF), V((2, OB, HQ, BT), BF),
        V((NZ, 1, 128), jnp.int32), V((NZ, 1, 128), F32), V((NDP, 1, 128), jnp.int32), V((NDP, 1, 128), F32),
        pltpu.SMEM((NDP, 1, 128), jnp.int32),
        V((8, 128), jnp.int32), pltpu.SMEM((8, 128), jnp.int32),
        V((8, 128), jnp.int32), pltpu.SMEM((8, 128), jnp.int32),
        V((8, 128), F32), V((NMP - 1, 8, 128), F32), V((2, SPD, 1, 128), F32),
        dma((5,)), dma((5,)), dma((MCH,)), dma((3,)),
        dma((2, CHUNKS, NMP - 1)), dma((2, CHUNKS, NMP - 1)),
        dma((2,)), dma((2,)), dma((2,)), dma((2,)), dma((2,)), dma((2,)),
        dma((2, NMP - 1)), dma((2, NMP - 1)), dma((NMP - 1,)), dma((NMP - 1,)),
    ]
    pred, logp, adv = pl.pallas_call(
        kernel,
        out_shape=(
            jax.ShapeDtypeStruct((OB, C, BT), BF),
            jax.ShapeDtypeStruct((1, 128), F32),
            jax.ShapeDtypeStruct((1, 128), F32),
        ),
        in_specs=[hbm] * 11,
        out_specs=(vmem, vmem, vmem),
        scratch_shapes=scratch,
        compiler_params=pltpu.CompilerParams(
            collective_id=0, has_side_effects=True, vmem_limit_bytes=48 * 1024 * 1024
        ),
        name="regroup_forward",
    )(
        *(
            pltpu.with_memory_space_constraint(a, pltpu.HBM)
            for a in (
                frames, owners, offsets, groups, rewards,
                norm_gain.reshape(D // 128, 128), latent, noise_blocks, embed_weight, mid_weight, head_weight.T,
            )
        )
    )
    return pred, logp[0, :SPD], adv[0, :SPD]


def solution(mesh):
    placed = (
        P("dp"), P("dp"), P("dp"), P("dp"), P("dp", None, None), P("dp", None, None), P("dp"),
        P(), P(), P(None, "mp"), P("mp", None),
    )
    return jax.shard_map(
        local,
        mesh=mesh,
        in_specs=placed,
        out_specs=(P("dp", None, None), P("dp"), P("dp")),
        check_vma=False,
    )
```

```python
import functools

import jax
import jax.numpy as jnp
from jax import lax
from jax.experimental import pallas as pl
from jax.experimental.pallas import tpu as pltpu
from jax.sharding import PartitionSpec as P

MESH = pl.DeviceIdType.MESH
D = 3072
C = 64
BT = 128
MAXB = 5
SPD = 6
SLOTS = 30
OB = 18
NY, NZ, NC = 4, 8, 2
NDP = NY * NZ * NC
NMP = 4
F = D // NMP
Q = C // NMP
HQ = Q // 2
MCH = 4
MSTEP = 6
PAIRS = SLOTS // 2
MROWS = D // MCH
RB = 256
CHUNKS = 5
CS = SLOTS // CHUNKS
OPEN = 2
SHARES = ((0, 0, OPEN),) + tuple((0, g, 1) for g in range(OPEN, CHUNKS)) + ((1, 0, 3), (1, 3, 2))
BF = jnp.bfloat16
F32 = jnp.float32


def far(k):
    z, y = (k // NC) % NZ, k // (NC * NZ)
    return min(z, NZ - z) + min(y, NY - y)


SHIFTS = sorted(range(1, NDP), key=far, reverse=True)


def peer_of(k):
    return lax.rem(lax.axis_index("dp") + k, NDP)


def kernel(
    frames_h, owners_h, offsets_h, groups_h, rewards_h,
    gain_h, latent_h, noise_h, embed_h, mid_h, head_h,
    pred_o, logp_o, adv_o,
    frames, owners, offsets, groups, rewards,
    ev, gv, mv, lat, noi, av, lw, ht, hb, act0, act1, act2, xs, xr, predb, pay, rcv0, rcv1, rows,
    izt, fzt, itab, ftab, stab, invv, invs, idxv, idxs, ext, exr, err,
    in_sem, s_sem, m_sem, loc_sem, xs_send, xs_recv, z_send, z_recv, meta_send, meta_recv, a2a_send, a2a_recv,
    ag_send, ag_recv, ex_send, ex_recv,
):
    me = lax.axis_index("dp")
    j = lax.axis_index("mp")
    barrier = pltpu.get_barrier_semaphore()

    c_e = pltpu.make_async_copy(embed_h, ev, in_sem.at[0])
    c_g = pltpu.make_async_copy(gain_h, gv, in_sem.at[1])
    c_h = pltpu.make_async_copy(head_h, ht, in_sem.at[2])
    c_l = pltpu.make_async_copy(latent_h, lat, in_sem.at[3])
    c_n = pltpu.make_async_copy(noise_h.at[:, pl.ds(pl.multiple_of(j * Q, Q), Q), :], noi, in_sem.at[4])
    c_m = [
        pltpu.make_async_copy(mid_h.at[pl.ds(k * MROWS, MROWS), :], mv.at[pl.ds(k * MROWS, MROWS), :], m_sem.at[k])
        for k in range(MCH)
    ]
    c_s = [
        pltpu.make_async_copy(src, dst, s_sem.at[k])
        for k, (src, dst) in enumerate(
            ((frames_h, frames), (owners_h, owners), (offsets_h, offsets), (groups_h, groups), (rewards_h, rewards))
        )
    ]
    c_e.start()
    c_g.start()
    c_l.start()
    for c in c_s:
        c.start()

    for d in range(1, NMP):
        pl.semaphore_signal(barrier, inc=1, device_id=(me, (j + d) % NMP), device_id_type=MESH)
    for i, k in enumerate(SHIFTS):
        pl.semaphore_signal(barrier, inc=1, device_id=(peer_of(k), j), device_id_type=MESH)
        if i % MSTEP == MSTEP - 1 and i // MSTEP < MCH:
            c_m[i // MSTEP].start()
    c_h.start()
    c_n.start()

    lane = lax.broadcasted_iota(jnp.int32, (8, 128), 1)
    sub = lax.broadcasted_iota(jnp.int32, (8, 128), 0)
    zi = (me // NC) % NZ
    yc = (me // (NZ * NC)) * NC + me % NC
    with jax.named_scope("index"):
        for c in c_s:
            c.wait()
        inv = jnp.zeros((8, 128), jnp.int32)
        off = jnp.full((8, 128), -1, jnp.int32)
        counts = jnp.ones((8, 128), jnp.int32)
        fm = jnp.zeros((8, 128), F32)
        gown = jnp.full((8, 128), -1, jnp.int32)
        own = jnp.zeros((8, 128), F32)
        for s in range(SPD):
            n = (frames[s] - 1) // 32 + 1
            counts = jnp.where(sub == s, n, counts)
            for k in range(MAXB):
                slot = s * MAXB + k
                hit = (lane == owners[slot]) & (k < n)
                inv = jnp.where(hit, slot, inv)
                off = jnp.where(hit, offsets[slot], off)
            off = jnp.where(lane == NDP + s, groups[s], off)
            fm = jnp.where(lane == NDP + s, rewards[s], fm)
            gown = jnp.where(sub == s, groups[s], gown)
            own = jnp.where(sub == s, rewards[s], own)
        off = jnp.where(lane >= NDP + SPD, -2, off)
        invv[...] = inv
        izt[zi] = off[0:1, :]
        fzt[zi] = fm[0:1, :]
        c_inv = pltpu.make_async_copy(invv, invs, loc_sem.at[0])
        c_inv.start()

    def pair(p):
        return jnp.concatenate([lat[2 * p], lat[2 * p + 1]], axis=1)

    def stack(x):
        return jnp.concatenate([x, x, x, x], axis=0)

    with jax.named_scope("norm"):
        c_e.wait()
        c_g.wait()
        for k in range(D // 128):
            cols = pl.ds(k * 128, 128)
            eg = ev[:, cols].astype(F32) * gv[k : k + 1, :]
            hi = eg.astype(BF)
            av[0:C, cols] = hi
            av[C : 2 * C, cols] = (eg - hi.astype(F32)).astype(BF)
        gram = jnp.zeros((C, 2 * C), F32)
        for k in range(2):
            e = ev[:, pl.ds(k * (D // 2), D // 2)]
            gram = gram + lax.dot_general(
                e, jnp.concatenate([e, e], axis=0), (((1,), (1,)), ((), ())), preferred_element_type=F32
            )
        g1 = gram.astype(BF).astype(F32)
        g2 = (gram - g1).astype(BF).astype(F32)
        g3 = gram - g1 - g2
        gl = lax.broadcasted_iota(jnp.int32, (C, 2 * C), 1)
        gparts = jnp.concatenate([jnp.where(gl < C, g1, g2), jnp.where(gl < C, g3, 0.0)], axis=1).astype(BF)
        c_l.wait()
        for p in range(SLOTS // 2):
            x = pair(p)
            gx = jnp.dot(gparts, stack(x), preferred_element_type=F32)
            sq = jnp.sum(x.astype(F32) * gx, axis=0, keepdims=True)
            hb[p] = 0.5 * lax.rsqrt(sq * (1.0 / D) + 0.25)

    with jax.named_scope("fold"):
        w = jnp.zeros((2 * C, F), F32)
        for k in range(2):
            for c in c_m[k * (MCH // 2) : (k + 1) * (MCH // 2)]:
                c.wait()
            ks = pl.ds(k * (D // 2), D // 2)
            w = w + jnp.dot(av[:, ks], mv[ks, :], preferred_element_type=F32)
        w = w[0:C, :] + w[C : 2 * C, :]
        whi = w.astype(BF).astype(F32)
        wst = jnp.concatenate([whi, w - whi], axis=0)
        lw[...] = jnp.transpose(wst).astype(BF)
        c_h.wait()

    def xcopy(h, g, n, d):
        to = (j + d) % NMP
        sl = pl.ds(g * CS, n * CS)
        return pltpu.make_async_remote_copy(
            src_ref=xs.at[h, to, sl], dst_ref=xr.at[h, d - 1, sl],
            send_sem=xs_send.at[h, g, d - 1], recv_sem=xs_recv.at[h, g, d - 1],
            device_id=(me, to), device_id_type=MESH,
        )

    def z_copies(k):
        to = (me // (NZ * NC)) * (NZ * NC) + lax.rem(zi + k, NZ) * NC + me % NC
        return [
            pltpu.make_async_remote_copy(
                src_ref=t.at[zi], dst_ref=t.at[zi], send_sem=z_send.at[i], recv_sem=z_recv.at[i],
                device_id=(to, j), device_id_type=MESH,
            )
            for i, t in enumerate((izt, fzt))
        ]

    def yc_copies(k):
        q = lax.rem(yc + k, NY * NC)
        to = (q // NC) * (NZ * NC) + zi * NC + q % NC
        return [
            pltpu.make_async_remote_copy(
                src_ref=t, dst_ref=tab.at[pl.ds(yc * NZ, NZ)], send_sem=meta_send.at[i], recv_sem=meta_recv.at[i],
                device_id=(to, j), device_id_type=MESH,
            )
            for i, (t, tab) in enumerate(((izt, itab), (fzt, ftab)))
        ]

    def all_of(ref, n, send, recv):
        return pltpu.make_async_remote_copy(
            src_ref=ref.at[pl.ds(0, n)], dst_ref=ref.at[pl.ds(0, n)], send_sem=send, recv_sem=recv,
            device_id=(me, (j + 1) % NMP), device_id_type=MESH,
        )

    acts = (act0, act1, act2)
    rcvs = (rcv0, rcv1)

    def hidden(p, act):
        x = pair(p)
        x2 = jnp.concatenate([x, x], axis=0)
        half = hb[p]
        for b in range(F // RB):
            rs = pl.ds(b * RB, RB)
            h = jnp.dot(lw[rs, :], x2, preferred_element_type=F32) * half
            act[rs, :] = (h + h * jnp.tanh(h)).astype(BF)

    def head(p, act):
        vel = jnp.dot(ht[...], act[...], preferred_element_type=F32).astype(BF)
        for q in range(NMP):
            for h in range(2):
                rs = slice(q * Q + h * HQ, q * Q + (h + 1) * HQ)
                xs[h, q, 2 * p] = vel[rs, 0:BT]
                xs[h, q, 2 * p + 1] = vel[rs, BT : 2 * BT]

    with jax.named_scope("forward"):
        hidden(0, act0)
        for p in range(PAIRS):
            if p + 1 < PAIRS:
                hidden(p + 1, acts[(p + 1) % len(acts)])
            head(p, acts[p % len(acts)])
            done = (2 * p + 2) // CS
            if (2 * p + 2) % CS == 0 and done >= OPEN:
                if done == OPEN:
                    pl.semaphore_wait(barrier, NDP - 1 + NMP - 1)
                    for k in range(1, NZ):
                        for c in z_copies(k):
                            c.start()
                for d in (2, 1, 3):
                    xcopy(*SHARES[done - OPEN], d).start()
        for share in SHARES:
            if share[0] == 1:
                for d in (2, 1, 3):
                    xcopy(*share, d).start()

    with jax.named_scope("meta"):
        all_of(izt, NZ - 1, z_send.at[0], z_recv.at[0]).wait_recv()
        all_of(fzt, NZ - 1, z_send.at[1], z_recv.at[1]).wait_recv()
        for k in range(1, NY * NC):
            for c in yc_copies(k):
                c.start()
        itab[pl.ds(yc * NZ, NZ)] = izt[...]
        ftab[pl.ds(yc * NZ, NZ)] = fzt[...]
        c_n.wait()

    def settle(h):
        for share in SHARES:
            if share[0] != h:
                continue
            for d in range(1, NMP):
                xcopy(*share, d).wait_recv()
            for slot in range(share[1] * CS, (share[1] + share[2]) * CS):
                v = xs[h, j, slot].astype(F32) + xr[h, 0, slot].astype(F32)
                v = v + (xr[h, 1, slot].astype(F32) + xr[h, 2, slot].astype(F32))
                predb[h, slot] = v.astype(BF)
                dlt = noi[slot, h * HQ : (h + 1) * HQ, :].astype(F32) + v
                err[h, slot] = dlt * dlt

    def send_blocks(h):
        for o in range(NDP):
            pay[h, o] = predb[h, invs[0, o]]
        for k in SHIFTS:
            p = peer_of(k)
            pltpu.make_async_remote_copy(
                src_ref=pay.at[h, p], dst_ref=rcvs[h].at[me], send_sem=a2a_send.at[h], recv_sem=a2a_recv.at[h],
                device_id=(p, j), device_id_type=MESH,
            ).start()
        rcvs[h][me] = pay[h, me]

    for h in range(2):
        with jax.named_scope("settle%d" % h):
            settle(h)
            if h == 0:
                c_inv.wait()
        with jax.named_scope("send_block%d" % h):
            send_blocks(h)

    et = jnp.zeros((8, 128), F32)
    for s in range(SPD):
        n = (frames[s] - 1) // 32 + 1
        acc = jnp.zeros((HQ, BT), F32)
        for k in range(MAXB):
            acc = acc + jnp.where(k < n, err[0, s * MAXB + k] + err[1, s * MAXB + k], 0.0)
        et = jnp.where(sub == s, jnp.sum(acc, axis=0, keepdims=True), et)
    ext[...] = et
    ex = [
        pltpu.make_async_remote_copy(
            src_ref=ext, dst_ref=exr.at[d - 1], send_sem=ex_send.at[d - 1], recv_sem=ex_recv.at[d - 1],
            device_id=(me, (j + d) % NMP), device_id_type=MESH,
        )
        for d in range(1, NMP)
    ]
    for c in ex:
        c.start()

    with jax.named_scope("tables"):
        all_of(itab, NDP - NZ, meta_send.at[0], meta_recv.at[0]).wait_recv()
        all_of(ftab, NDP - NZ, meta_send.at[1], meta_recv.at[1]).wait_recv()
        c_tab = pltpu.make_async_copy(itab, stab, loc_sem.at[1])
        c_tab.start()

        def prompt(s, carry):
            a, b = carry
            hit = gown == itab[s]
            r = jnp.where(hit & (lane >= NDP), jnp.broadcast_to(ftab[s], (8, 128)), 0.0)
            return a + r, b + r * r

        zero = jnp.zeros((8, 128), F32)
        gsum, gsq = lax.fori_loop(0, NDP, prompt, (zero, zero))
        mean = jnp.sum(gsum, axis=1, keepdims=True) * (1.0 / 12.0)
        var = jnp.sum(gsq, axis=1, keepdims=True) * (1.0 / 12.0) - mean * mean
        adv = (own - mean) / jnp.sqrt(var + 0.25)
        adv_o[...] = jnp.sum(jnp.where(lane == sub, adv, 0.0), axis=0, keepdims=True)
        c_tab.wait()
        idx = jnp.zeros((8, 128), jnp.int32)
        for s in range(NDP):
            src = (s // NZ // NC) * (NZ * NC) + (s % NZ) * NC + (s // NZ) % NC
            idx = jnp.where(lane == stab[s, 0, me], src, idx)
        idxv[...] = idx
        c_idx = pltpu.make_async_copy(idxv, idxs, loc_sem.at[2])
        c_idx.start()
        c_idx.wait()

    def gather_copy(h, d):
        return pltpu.make_async_remote_copy(
            src_ref=rows.at[h], dst_ref=pred_o.at[:, pl.ds(pl.multiple_of(j * Q + h * HQ, HQ), HQ), :],
            send_sem=ag_send.at[h, d - 1], recv_sem=ag_recv.at[h, d - 1],
            device_id=(me, (j + d) % NMP), device_id_type=MESH,
        )

    for h in range(2):
        with jax.named_scope("a2a_wait%d" % h):
            all_of(rcvs[h], NDP - 1, a2a_send.at[h], a2a_recv.at[h]).wait_recv()
        for r in range(OB):
            block = rcvs[h][idxs[0, r]]
            rows[h, r] = block
            pred_o[r, pl.ds(pl.multiple_of(j * Q + h * HQ, HQ), HQ), :] = block
        for d in (2, 1, 3):
            gather_copy(h, d).start()
        if h == 0:
            for c in ex:
                c.wait_recv()
            tot = jnp.sum(ext[...] + exr[0] + (exr[1] + exr[2]), axis=1, keepdims=True)
            lp = -0.5 * tot / (counts * (BT * C)).astype(F32)
            logp_o[...] = jnp.sum(jnp.where(lane == sub, lp, 0.0), axis=0, keepdims=True)

    with jax.named_scope("final_wait"):
        all_of(izt, NZ - 1, z_send.at[0], z_recv.at[0]).wait_send()
        all_of(fzt, NZ - 1, z_send.at[1], z_recv.at[1]).wait_send()
        all_of(itab, NDP - NZ, meta_send.at[0], meta_recv.at[0]).wait_send()
        all_of(ftab, NDP - NZ, meta_send.at[1], meta_recv.at[1]).wait_send()
        for share in SHARES:
            for d in range(1, NMP):
                xcopy(*share, d).wait_send()
        for c in ex:
            c.wait_send()
        for h in range(2):
            all_of(rcvs[h], NDP - 1, a2a_send.at[h], a2a_recv.at[h]).wait_send()
            for d in range(1, NMP):
                gather_copy(h, d).wait()


def local(
    frames, owners, offsets, groups, latent, noise_blocks, rewards, embed_weight, norm_gain, mid_weight, head_weight
):
    hbm = pl.BlockSpec(memory_space=pl.ANY)
    vmem = pl.BlockSpec(memory_space=pltpu.VMEM)
    dma = pltpu.SemaphoreType.DMA
    V = pltpu.VMEM
    S = pltpu.SMEM
    scratch = [
        S((SPD,), jnp.int32), S((SLOTS,), jnp.int32), S((SLOTS,), jnp.int32), S((SPD,), jnp.int32), S((SPD,), F32),
        V((C, D), BF), V((D // 128, 128), F32), V((D, F), BF),
        V((SLOTS, C, BT), BF), V((SLOTS, Q, BT), BF),
        V((2 * C, D), BF), V((F, 2 * C), BF), V((C, F), BF),
        V((SLOTS // 2, 1, 2 * BT), F32), V((F, 2 * BT), BF), V((F, 2 * BT), BF), V((F, 2 * BT), BF),
        V((2, NMP, SLOTS, HQ, BT), BF), V((2, NMP - 1, SLOTS, HQ, BT), BF),
        V((2, SLOTS, HQ, BT), BF), V((2, NDP, HQ, BT), BF), V((NDP, HQ, BT), BF), V((NDP, HQ, BT), BF), V((2, OB, HQ, BT), BF),
        V((NZ, 1, 128), jnp.int32), V((NZ, 1, 128), F32), V((NDP, 1, 128), jnp.int32), V((NDP, 1, 128), F32),
        pltpu.SMEM((NDP, 1, 128), jnp.int32),
        V((8, 128), jnp.int32), pltpu.SMEM((8, 128), jnp.int32),
        V((8, 128), jnp.int32), pltpu.SMEM((8, 128), jnp.int32),
        V((8, 128), F32), V((NMP - 1, 8, 128), F32), V((2, SLOTS, HQ, BT), F32),
        dma((5,)), dma((5,)), dma((MCH,)), dma((3,)),
        dma((2, CHUNKS, NMP - 1)), dma((2, CHUNKS, NMP - 1)),
        dma((2,)), dma((2,)), dma((2,)), dma((2,)), dma((2,)), dma((2,)),
        dma((2, NMP - 1)), dma((2, NMP - 1)), dma((NMP - 1,)), dma((NMP - 1,)),
    ]
    pred, logp, adv = pl.pallas_call(
        kernel,
        out_shape=(
            jax.ShapeDtypeStruct((OB, C, BT), BF),
            jax.ShapeDtypeStruct((1, 128), F32),
            jax.ShapeDtypeStruct((1, 128), F32),
        ),
        in_specs=[hbm] * 11,
        out_specs=(vmem, vmem, vmem),
        scratch_shapes=scratch,
        compiler_params=pltpu.CompilerParams(
            collective_id=0, has_side_effects=True, vmem_limit_bytes=48 * 1024 * 1024
        ),
        name="regroup_forward",
    )(
        *(
            pltpu.with_memory_space_constraint(a, pltpu.HBM)
            for a in (
                frames, owners, offsets, groups, rewards,
                norm_gain.reshape(D // 128, 128), latent, noise_blocks, embed_weight, mid_weight, head_weight.T,
            )
        )
    )
    return pred, logp[0, :SPD], adv[0, :SPD]


def solution(mesh):
    placed = (
        P("dp"), P("dp"), P("dp"), P("dp"), P("dp", None, None), P("dp", None, None), P("dp"),
        P(), P(), P(None, "mp"), P("mp", None),
    )
    return jax.shard_map(
        local,
        mesh=mesh,
        in_specs=placed,
        out_specs=(P("dp", None, None), P("dp"), P("dp")),
        check_vma=False,
    )
```

```python
import functools

import jax
import jax.numpy as jnp
from jax import lax
from jax.experimental import pallas as pl
from jax.experimental.pallas import tpu as pltpu
from jax.sharding import PartitionSpec as P

MESH = pl.DeviceIdType.MESH
D = 3072
C = 64
BT = 128
MAXB = 5
SPD = 6
SLOTS = 30
OB = 18
NY, NZ, NC = 4, 8, 2
NDP = NY * NZ * NC
NMP = 4
F = D // NMP
Q = C // NMP
HQ = Q // 2
MCH = 4
MSTEP = 6
PAIRS = SLOTS // 2
MROWS = D // MCH
RB = 256
CHUNKS = 5
CS = SLOTS // CHUNKS
OPEN = 1
SHARES = ((0, 0, OPEN),) + tuple((0, g, 1) for g in range(OPEN, CHUNKS)) + ((1, 0, 3), (1, 3, 2))
BF = jnp.bfloat16
F32 = jnp.float32


def far(k):
    z, y = (k // NC) % NZ, k // (NC * NZ)
    return min(z, NZ - z) + min(y, NY - y)


SHIFTS = sorted(range(1, NDP), key=far, reverse=True)


def peer_of(k):
    return lax.rem(lax.axis_index("dp") + k, NDP)


def kernel(
    frames_h, owners_h, offsets_h, groups_h, rewards_h,
    gain_h, latent_h, noise_h, embed_h, mid_h, head_h,
    pred_o, logp_o, adv_o,
    frames, owners, offsets, groups, rewards,
    ev, gv, mv, lat, noi, av, lw, ht, hb, act0, act1, act2, xs, xr, predb, pay, rcv0, rcv1, rows,
    izt, fzt, itab, ftab, stab, invv, invs, idxv, idxs, ext, exr, err,
    in_sem, s_sem, m_sem, loc_sem, xs_send, xs_recv, z_send, z_recv, meta_send, meta_recv, a2a_send, a2a_recv,
    ag_send, ag_recv, ex_send, ex_recv,
):
    me = lax.axis_index("dp")
    j = lax.axis_index("mp")
    barrier = pltpu.get_barrier_semaphore()

    c_e = pltpu.make_async_copy(embed_h, ev, in_sem.at[0])
    c_g = pltpu.make_async_copy(gain_h, gv, in_sem.at[1])
    c_h = pltpu.make_async_copy(head_h, ht, in_sem.at[2])
    c_l = pltpu.make_async_copy(latent_h, lat, in_sem.at[3])
    c_n = pltpu.make_async_copy(noise_h.at[:, pl.ds(pl.multiple_of(j * Q, Q), Q), :], noi, in_sem.at[4])
    c_m = [
        pltpu.make_async_copy(mid_h.at[pl.ds(k * MROWS, MROWS), :], mv.at[pl.ds(k * MROWS, MROWS), :], m_sem.at[k])
        for k in range(MCH)
    ]
    c_s = [
        pltpu.make_async_copy(src, dst, s_sem.at[k])
        for k, (src, dst) in enumerate(
            ((frames_h, frames), (owners_h, owners), (offsets_h, offsets), (groups_h, groups), (rewards_h, rewards))
        )
    ]
    c_e.start()
    c_g.start()
    c_l.start()
    for c in c_s:
        c.start()

    for d in range(1, NMP):
        pl.semaphore_signal(barrier, inc=1, device_id=(me, (j + d) % NMP), device_id_type=MESH)
    for i, k in enumerate(SHIFTS):
        pl.semaphore_signal(barrier, inc=1, device_id=(peer_of(k), j), device_id_type=MESH)
        if i % MSTEP == MSTEP - 1 and i // MSTEP < MCH:
            c_m[i // MSTEP].start()
    c_h.start()
    c_n.start()

    lane = lax.broadcasted_iota(jnp.int32, (8, 128), 1)
    sub = lax.broadcasted_iota(jnp.int32, (8, 128), 0)
    zi = (me // NC) % NZ
    yc = (me // (NZ * NC)) * NC + me % NC
    with jax.named_scope("index"):
        for c in c_s:
            c.wait()
        inv = jnp.zeros((8, 128), jnp.int32)
        off = jnp.full((8, 128), -1, jnp.int32)
        counts = jnp.ones((8, 128), jnp.int32)
        fm = jnp.zeros((8, 128), F32)
        gown = jnp.full((8, 128), -1, jnp.int32)
        own = jnp.zeros((8, 128), F32)
        for s in range(SPD):
            n = (frames[s] - 1) // 32 + 1
            counts = jnp.where(sub == s, n, counts)
            for k in range(MAXB):
                slot = s * MAXB + k
                hit = (lane == owners[slot]) & (k < n)
                inv = jnp.where(hit, slot, inv)
                off = jnp.where(hit, offsets[slot], off)
            off = jnp.where(lane == NDP + s, groups[s], off)
            fm = jnp.where(lane == NDP + s, rewards[s], fm)
            gown = jnp.where(sub == s, groups[s], gown)
            own = jnp.where(sub == s, rewards[s], own)
        off = jnp.where(lane >= NDP + SPD, -2, off)
        invv[...] = inv
        izt[zi] = off[0:1, :]
        fzt[zi] = fm[0:1, :]
        c_inv = pltpu.make_async_copy(invv, invs, loc_sem.at[0])
        c_inv.start()

    def pair(p):
        return jnp.concatenate([lat[2 * p], lat[2 * p + 1]], axis=1)

    def stack(x):
        return jnp.concatenate([x, x, x, x], axis=0)

    with jax.named_scope("norm"):
        c_e.wait()
        c_g.wait()
        for k in range(D // 128):
            cols = pl.ds(k * 128, 128)
            eg = ev[:, cols].astype(F32) * gv[k : k + 1, :]
            hi = eg.astype(BF)
            av[0:C, cols] = hi
            av[C : 2 * C, cols] = (eg - hi.astype(F32)).astype(BF)
        gram = jnp.zeros((C, 2 * C), F32)
        for k in range(2):
            e = ev[:, pl.ds(k * (D // 2), D // 2)]
            gram = gram + lax.dot_general(
                e, jnp.concatenate([e, e], axis=0), (((1,), (1,)), ((), ())), preferred_element_type=F32
            )
        g1 = gram.astype(BF).astype(F32)
        g2 = (gram - g1).astype(BF).astype(F32)
        g3 = gram - g1 - g2
        gl = lax.broadcasted_iota(jnp.int32, (C, 2 * C), 1)
        gparts = jnp.concatenate([jnp.where(gl < C, g1, g2), jnp.where(gl < C, g3, 0.0)], axis=1).astype(BF)
        c_l.wait()
        for p in range(SLOTS // 2):
            x = pair(p)
            gx = jnp.dot(gparts, stack(x), preferred_element_type=F32)
            sq = jnp.sum(x.astype(F32) * gx, axis=0, keepdims=True)
            hb[p] = 0.5 * lax.rsqrt(sq * (1.0 / D) + 0.25)

    with jax.named_scope("fold"):
        w = jnp.zeros((2 * C, F), F32)
        for k in range(2):
            for c in c_m[k * (MCH // 2) : (k + 1) * (MCH // 2)]:
                c.wait()
            ks = pl.ds(k * (D // 2), D // 2)
            w = w + jnp.dot(av[:, ks], mv[ks, :], preferred_element_type=F32)
        w = w[0:C, :] + w[C : 2 * C, :]
        whi = w.astype(BF).astype(F32)
        wst = jnp.concatenate([whi, w - whi], axis=0)
        lw[...] = jnp.transpose(wst).astype(BF)
        c_h.wait()

    def xcopy(h, g, n, d):
        to = (j + d) % NMP
        sl = pl.ds(g * CS, n * CS)
        return pltpu.make_async_remote_copy(
            src_ref=xs.at[h, to, sl], dst_ref=xr.at[h, d - 1, sl],
            send_sem=xs_send.at[h, g, d - 1], recv_sem=xs_recv.at[h, g, d - 1],
            device_id=(me, to), device_id_type=MESH,
        )

    def z_copies(k):
        to = (me // (NZ * NC)) * (NZ * NC) + lax.rem(zi + k, NZ) * NC + me % NC
        return [
            pltpu.make_async_remote_copy(
                src_ref=t.at[zi], dst_ref=t.at[zi], send_sem=z_send.at[i], recv_sem=z_recv.at[i],
                device_id=(to, j), device_id_type=MESH,
            )
            for i, t in enumerate((izt, fzt))
        ]

    def yc_copies(k):
        q = lax.rem(yc + k, NY * NC)
        to = (q // NC) * (NZ * NC) + zi * NC + q % NC
        return [
            pltpu.make_async_remote_copy(
                src_ref=t, dst_ref=tab.at[pl.ds(yc * NZ, NZ)], send_sem=meta_send.at[i], recv_sem=meta_recv.at[i],
                device_id=(to, j), device_id_type=MESH,
            )
            for i, (t, tab) in enumerate(((izt, itab), (fzt, ftab)))
        ]

    def all_of(ref, n, send, recv):
        return pltpu.make_async_remote_copy(
            src_ref=ref.at[pl.ds(0, n)], dst_ref=ref.at[pl.ds(0, n)], send_sem=send, recv_sem=recv,
            device_id=(me, (j + 1) % NMP), device_id_type=MESH,
        )

    acts = (act0, act1, act2)
    rcvs = (rcv0, rcv1)

    def hidden(p, act):
        x = pair(p)
        x2 = jnp.concatenate([x, x], axis=0)
        half = hb[p]
        for b in range(F // RB):
            rs = pl.ds(b * RB, RB)
            h = jnp.dot(lw[rs, :], x2, preferred_element_type=F32) * half
            act[rs, :] = (h + h * jnp.tanh(h)).astype(BF)

    def head(p, act):
        vel = jnp.dot(ht[...], act[...], preferred_element_type=F32).astype(BF)
        for q in range(NMP):
            for h in range(2):
                rs = slice(q * Q + h * HQ, q * Q + (h + 1) * HQ)
                xs[h, q, 2 * p] = vel[rs, 0:BT]
                xs[h, q, 2 * p + 1] = vel[rs, BT : 2 * BT]

    with jax.named_scope("forward"):
        hidden(0, act0)
        for p in range(PAIRS):
            if p + 1 < PAIRS:
                hidden(p + 1, acts[(p + 1) % len(acts)])
            head(p, acts[p % len(acts)])
            done = (2 * p + 2) // CS
            if (2 * p + 2) % CS == 0 and done >= OPEN:
                if done == OPEN:
                    pl.semaphore_wait(barrier, NDP - 1 + NMP - 1)
                    for k in range(1, NZ):
                        for c in z_copies(k):
                            c.start()
                for d in (2, 1, 3):
                    xcopy(*SHARES[done - OPEN], d).start()
        for share in SHARES:
            if share[0] == 1:
                for d in (2, 1, 3):
                    xcopy(*share, d).start()

    with jax.named_scope("meta"):
        all_of(izt, NZ - 1, z_send.at[0], z_recv.at[0]).wait_recv()
        all_of(fzt, NZ - 1, z_send.at[1], z_recv.at[1]).wait_recv()
        for k in range(1, NY * NC):
            for c in yc_copies(k):
                c.start()
        itab[pl.ds(yc * NZ, NZ)] = izt[...]
        ftab[pl.ds(yc * NZ, NZ)] = fzt[...]
        c_n.wait()

    def settle(h):
        for share in SHARES:
            if share[0] != h:
                continue
            for d in range(1, NMP):
                xcopy(*share, d).wait_recv()
            for slot in range(share[1] * CS, (share[1] + share[2]) * CS):
                v = xs[h, j, slot].astype(F32) + xr[h, 0, slot].astype(F32)
                v = v + (xr[h, 1, slot].astype(F32) + xr[h, 2, slot].astype(F32))
                predb[h, slot] = v.astype(BF)
                dlt = noi[slot, h * HQ : (h + 1) * HQ, :].astype(F32) + v
                err[h, slot] = dlt * dlt

    def send_blocks(h):
        for o in range(NDP):
            pay[h, o] = predb[h, invs[0, o]]
        for k in SHIFTS:
            p = peer_of(k)
            pltpu.make_async_remote_copy(
                src_ref=pay.at[h, p], dst_ref=rcvs[h].at[me], send_sem=a2a_send.at[h], recv_sem=a2a_recv.at[h],
                device_id=(p, j), device_id_type=MESH,
            ).start()
        rcvs[h][me] = pay[h, me]

    for h in range(2):
        with jax.named_scope("settle%d" % h):
            settle(h)
            if h == 0:
                c_inv.wait()
        with jax.named_scope("send_block%d" % h):
            send_blocks(h)

    et = jnp.zeros((8, 128), F32)
    for s in range(SPD):
        n = (frames[s] - 1) // 32 + 1
        acc = jnp.zeros((HQ, BT), F32)
        for k in range(MAXB):
            acc = acc + jnp.where(k < n, err[0, s * MAXB + k] + err[1, s * MAXB + k], 0.0)
        et = jnp.where(sub == s, jnp.sum(acc, axis=0, keepdims=True), et)
    ext[...] = et
    ex = [
        pltpu.make_async_remote_copy(
            src_ref=ext, dst_ref=exr.at[d - 1], send_sem=ex_send.at[d - 1], recv_sem=ex_recv.at[d - 1],
            device_id=(me, (j + d) % NMP), device_id_type=MESH,
        )
        for d in range(1, NMP)
    ]
    for c in ex:
        c.start()

    with jax.named_scope("tables"):
        all_of(itab, NDP - NZ, meta_send.at[0], meta_recv.at[0]).wait_recv()
        all_of(ftab, NDP - NZ, meta_send.at[1], meta_recv.at[1]).wait_recv()
        c_tab = pltpu.make_async_copy(itab, stab, loc_sem.at[1])
        c_tab.start()

        def prompt(s, carry):
            a, b = carry
            hit = gown == itab[s]
            r = jnp.where(hit & (lane >= NDP), jnp.broadcast_to(ftab[s], (8, 128)), 0.0)
            return a + r, b + r * r

        zero = jnp.zeros((8, 128), F32)
        gsum, gsq = lax.fori_loop(0, NDP, prompt, (zero, zero))
        mean = jnp.sum(gsum, axis=1, keepdims=True) * (1.0 / 12.0)
        var = jnp.sum(gsq, axis=1, keepdims=True) * (1.0 / 12.0) - mean * mean
        adv = (own - mean) / jnp.sqrt(var + 0.25)
        adv_o[...] = jnp.sum(jnp.where(lane == sub, adv, 0.0), axis=0, keepdims=True)
        c_tab.wait()
        idx = jnp.zeros((8, 128), jnp.int32)
        for s in range(NDP):
            src = (s // NZ // NC) * (NZ * NC) + (s % NZ) * NC + (s // NZ) % NC
            idx = jnp.where(lane == stab[s, 0, me], src, idx)
        idxv[...] = idx
        c_idx = pltpu.make_async_copy(idxv, idxs, loc_sem.at[2])
        c_idx.start()
        c_idx.wait()

    def gather_copy(h, d):
        return pltpu.make_async_remote_copy(
            src_ref=rows.at[h], dst_ref=pred_o.at[:, pl.ds(pl.multiple_of(j * Q + h * HQ, HQ), HQ), :],
            send_sem=ag_send.at[h, d - 1], recv_sem=ag_recv.at[h, d - 1],
            device_id=(me, (j + d) % NMP), device_id_type=MESH,
        )

    for h in range(2):
        with jax.named_scope("a2a_wait%d" % h):
            all_of(rcvs[h], NDP - 1, a2a_send.at[h], a2a_recv.at[h]).wait_recv()
        for r in range(OB):
            block = rcvs[h][idxs[0, r]]
            rows[h, r] = block
            pred_o[r, pl.ds(pl.multiple_of(j * Q + h * HQ, HQ), HQ), :] = block
        for d in (2, 1, 3):
            gather_copy(h, d).start()
        if h == 0:
            for c in ex:
                c.wait_recv()
            tot = jnp.sum(ext[...] + exr[0] + (exr[1] + exr[2]), axis=1, keepdims=True)
            lp = -0.5 * tot / (counts * (BT * C)).astype(F32)
            logp_o[...] = jnp.sum(jnp.where(lane == sub, lp, 0.0), axis=0, keepdims=True)

    with jax.named_scope("final_wait"):
        all_of(izt, NZ - 1, z_send.at[0], z_recv.at[0]).wait_send()
        all_of(fzt, NZ - 1, z_send.at[1], z_recv.at[1]).wait_send()
        all_of(itab, NDP - NZ, meta_send.at[0], meta_recv.at[0]).wait_send()
        all_of(ftab, NDP - NZ, meta_send.at[1], meta_recv.at[1]).wait_send()
        for share in SHARES:
            for d in range(1, NMP):
                xcopy(*share, d).wait_send()
        for c in ex:
            c.wait_send()
        for h in range(2):
            all_of(rcvs[h], NDP - 1, a2a_send.at[h], a2a_recv.at[h]).wait_send()
            for d in range(1, NMP):
                gather_copy(h, d).wait()


def local(
    frames, owners, offsets, groups, latent, noise_blocks, rewards, embed_weight, norm_gain, mid_weight, head_weight
):
    hbm = pl.BlockSpec(memory_space=pl.ANY)
    vmem = pl.BlockSpec(memory_space=pltpu.VMEM)
    dma = pltpu.SemaphoreType.DMA
    V = pltpu.VMEM
    S = pltpu.SMEM
    scratch = [
        S((SPD,), jnp.int32), S((SLOTS,), jnp.int32), S((SLOTS,), jnp.int32), S((SPD,), jnp.int32), S((SPD,), F32),
        V((C, D), BF), V((D // 128, 128), F32), V((D, F), BF),
        V((SLOTS, C, BT), BF), V((SLOTS, Q, BT), BF),
        V((2 * C, D), BF), V((F, 2 * C), BF), V((C, F), BF),
        V((SLOTS // 2, 1, 2 * BT), F32), V((F, 2 * BT), BF), V((F, 2 * BT), BF), V((F, 2 * BT), BF),
        V((2, NMP, SLOTS, HQ, BT), BF), V((2, NMP - 1, SLOTS, HQ, BT), BF),
        V((2, SLOTS, HQ, BT), BF), V((2, NDP, HQ, BT), BF), V((NDP, HQ, BT), BF), V((NDP, HQ, BT), BF), V((2, OB, HQ, BT), BF),
        V((NZ, 1, 128), jnp.int32), V((NZ, 1, 128), F32), V((NDP, 1, 128), jnp.int32), V((NDP, 1, 128), F32),
        pltpu.SMEM((NDP, 1, 128), jnp.int32),
        V((8, 128), jnp.int32), pltpu.SMEM((8, 128), jnp.int32),
        V((8, 128), jnp.int32), pltpu.SMEM((8, 128), jnp.int32),
        V((8, 128), F32), V((NMP - 1, 8, 128), F32), V((2, SLOTS, HQ, BT), F32),
        dma((5,)), dma((5,)), dma((MCH,)), dma((3,)),
        dma((2, CHUNKS, NMP - 1)), dma((2, CHUNKS, NMP - 1)),
        dma((2,)), dma((2,)), dma((2,)), dma((2,)), dma((2,)), dma((2,)),
        dma((2, NMP - 1)), dma((2, NMP - 1)), dma((NMP - 1,)), dma((NMP - 1,)),
    ]
    pred, logp, adv = pl.pallas_call(
        kernel,
        out_shape=(
            jax.ShapeDtypeStruct((OB, C, BT), BF),
            jax.ShapeDtypeStruct((1, 128), F32),
            jax.ShapeDtypeStruct((1, 128), F32),
        ),
        in_specs=[hbm] * 11,
        out_specs=(vmem, vmem, vmem),
        scratch_shapes=scratch,
        compiler_params=pltpu.CompilerParams(
            collective_id=0, has_side_effects=True, vmem_limit_bytes=48 * 1024 * 1024
        ),
        name="regroup_forward",
    )(
        *(
            pltpu.with_memory_space_constraint(a, pltpu.HBM)
            for a in (
                frames, owners, offsets, groups, rewards,
                norm_gain.reshape(D // 128, 128), latent, noise_blocks, embed_weight, mid_weight, head_weight.T,
            )
        )
    )
    return pred, logp[0, :SPD], adv[0, :SPD]


def solution(mesh):
    placed = (
        P("dp"), P("dp"), P("dp"), P("dp"), P("dp", None, None), P("dp", None, None), P("dp"),
        P(), P(), P(None, "mp"), P("mp", None),
    )
    return jax.shard_map(
        local,
        mesh=mesh,
        in_specs=placed,
        out_specs=(P("dp", None, None), P("dp"), P("dp")),
        check_vma=False,
    )
```

```python
import functools

import jax
import jax.numpy as jnp
from jax import lax
from jax.experimental import pallas as pl
from jax.experimental.pallas import tpu as pltpu
from jax.sharding import PartitionSpec as P

MESH = pl.DeviceIdType.MESH
D = 3072
C = 64
BT = 128
MAXB = 5
SPD = 6
SLOTS = 30
OB = 18
NY, NZ, NC = 4, 8, 2
NDP = NY * NZ * NC
NMP = 4
F = D // NMP
Q = C // NMP
HQ = Q // 2
MCH = 4
MSTEP = 6
PAIRS = SLOTS // 2
MROWS = D // MCH
RB = 192
CHUNKS = 5
CS = SLOTS // CHUNKS
OPEN = 1
SHARES = ((0, 0, OPEN),) + tuple((0, g, 1) for g in range(OPEN, CHUNKS)) + ((1, 0, 3), (1, 3, 2))
BF = jnp.bfloat16
F32 = jnp.float32


def far(k):
    z, y = (k // NC) % NZ, k // (NC * NZ)
    return min(z, NZ - z) + min(y, NY - y)


SHIFTS = sorted(range(1, NDP), key=far, reverse=True)


def peer_of(k):
    return lax.rem(lax.axis_index("dp") + k, NDP)


def kernel(
    frames_h, owners_h, offsets_h, groups_h, rewards_h,
    gain_h, latent_h, noise_h, embed_h, mid_h, head_h,
    pred_o, logp_o, adv_o,
    frames, owners, offsets, groups, rewards,
    ev, gv, mv, lat, noi, av, lw, ht, hb, act0, act1, act2, xs, xr, predb, pay, rcv0, rcv1, rows,
    izt, fzt, itab, ftab, stab, invv, invs, idxv, idxs, ext, exr, err,
    in_sem, s_sem, m_sem, loc_sem, xs_send, xs_recv, z_send, z_recv, meta_send, meta_recv, a2a_send, a2a_recv,
    ag_send, ag_recv, ex_send, ex_recv,
):
    me = lax.axis_index("dp")
    j = lax.axis_index("mp")
    barrier = pltpu.get_barrier_semaphore()

    c_e = pltpu.make_async_copy(embed_h, ev, in_sem.at[0])
    c_g = pltpu.make_async_copy(gain_h, gv, in_sem.at[1])
    c_h = pltpu.make_async_copy(head_h, ht, in_sem.at[2])
    c_l = pltpu.make_async_copy(latent_h, lat, in_sem.at[3])
    c_n = pltpu.make_async_copy(noise_h.at[:, pl.ds(pl.multiple_of(j * Q, Q), Q), :], noi, in_sem.at[4])
    c_m = [
        pltpu.make_async_copy(mid_h.at[pl.ds(k * MROWS, MROWS), :], mv.at[pl.ds(k * MROWS, MROWS), :], m_sem.at[k])
        for k in range(MCH)
    ]
    c_s = [
        pltpu.make_async_copy(src, dst, s_sem.at[k])
        for k, (src, dst) in enumerate(
            ((frames_h, frames), (owners_h, owners), (offsets_h, offsets), (groups_h, groups), (rewards_h, rewards))
        )
    ]
    c_e.start()
    c_g.start()
    c_l.start()
    for c in c_s:
        c.start()

    for d in range(1, NMP):
        pl.semaphore_signal(barrier, inc=1, device_id=(me, (j + d) % NMP), device_id_type=MESH)
    for i, k in enumerate(SHIFTS):
        pl.semaphore_signal(barrier, inc=1, device_id=(peer_of(k), j), device_id_type=MESH)
        if i % MSTEP == MSTEP - 1 and i // MSTEP < MCH:
            c_m[i // MSTEP].start()
    c_h.start()
    c_n.start()

    lane = lax.broadcasted_iota(jnp.int32, (8, 128), 1)
    sub = lax.broadcasted_iota(jnp.int32, (8, 128), 0)
    zi = (me // NC) % NZ
    yc = (me // (NZ * NC)) * NC + me % NC
    with jax.named_scope("index"):
        for c in c_s:
            c.wait()
        inv = jnp.zeros((8, 128), jnp.int32)
        off = jnp.full((8, 128), -1, jnp.int32)
        counts = jnp.ones((8, 128), jnp.int32)
        fm = jnp.zeros((8, 128), F32)
        gown = jnp.full((8, 128), -1, jnp.int32)
        own = jnp.zeros((8, 128), F32)
        for s in range(SPD):
            n = (frames[s] - 1) // 32 + 1
            counts = jnp.where(sub == s, n, counts)
            for k in range(MAXB):
                slot = s * MAXB + k
                hit = (lane == owners[slot]) & (k < n)
                inv = jnp.where(hit, slot, inv)
                off = jnp.where(hit, offsets[slot], off)
            off = jnp.where(lane == NDP + s, groups[s], off)
            fm = jnp.where(lane == NDP + s, rewards[s], fm)
            gown = jnp.where(sub == s, groups[s], gown)
            own = jnp.where(sub == s, rewards[s], own)
        off = jnp.where(lane >= NDP + SPD, -2, off)
        invv[...] = inv
        izt[zi] = off[0:1, :]
        fzt[zi] = fm[0:1, :]
        c_inv = pltpu.make_async_copy(invv, invs, loc_sem.at[0])
        c_inv.start()

    def pair(p):
        return jnp.concatenate([lat[2 * p], lat[2 * p + 1]], axis=1)

    def stack(x):
        return jnp.concatenate([x, x, x, x], axis=0)

    with jax.named_scope("norm"):
        c_e.wait()
        c_g.wait()
        for k in range(D // 128):
            cols = pl.ds(k * 128, 128)
            eg = ev[:, cols].astype(F32) * gv[k : k + 1, :]
            hi = eg.astype(BF)
            av[0:C, cols] = hi
            av[C : 2 * C, cols] = (eg - hi.astype(F32)).astype(BF)
        gram = jnp.zeros((C, 2 * C), F32)
        for k in range(2):
            e = ev[:, pl.ds(k * (D // 2), D // 2)]
            gram = gram + lax.dot_general(
                e, jnp.concatenate([e, e], axis=0), (((1,), (1,)), ((), ())), preferred_element_type=F32
            )
        g1 = gram.astype(BF).astype(F32)
        g2 = (gram - g1).astype(BF).astype(F32)
        g3 = gram - g1 - g2
        gl = lax.broadcasted_iota(jnp.int32, (C, 2 * C), 1)
        gparts = jnp.concatenate([jnp.where(gl < C, g1, g2), jnp.where(gl < C, g3, 0.0)], axis=1).astype(BF)
        c_l.wait()
        for p in range(SLOTS // 2):
            x = pair(p)
            gx = jnp.dot(gparts, stack(x), preferred_element_type=F32)
            sq = jnp.sum(x.astype(F32) * gx, axis=0, keepdims=True)
            hb[p] = 0.5 * lax.rsqrt(sq * (1.0 / D) + 0.25)

    with jax.named_scope("fold"):
        w = jnp.zeros((2 * C, F), F32)
        for k in range(2):
            for c in c_m[k * (MCH // 2) : (k + 1) * (MCH // 2)]:
                c.wait()
            ks = pl.ds(k * (D // 2), D // 2)
            w = w + jnp.dot(av[:, ks], mv[ks, :], preferred_element_type=F32)
        w = w[0:C, :] + w[C : 2 * C, :]
        whi = w.astype(BF).astype(F32)
        wst = jnp.concatenate([whi, w - whi], axis=0)
        lw[...] = jnp.transpose(wst).astype(BF)
        c_h.wait()

    def xcopy(h, g, n, d):
        to = (j + d) % NMP
        sl = pl.ds(g * CS, n * CS)
        return pltpu.make_async_remote_copy(
            src_ref=xs.at[h, to, sl], dst_ref=xr.at[h, d - 1, sl],
            send_sem=xs_send.at[h, g, d - 1], recv_sem=xs_recv.at[h, g, d - 1],
            device_id=(me, to), device_id_type=MESH,
        )

    def z_copies(k):
        to = (me // (NZ * NC)) * (NZ * NC) + lax.rem(zi + k, NZ) * NC + me % NC
        return [
            pltpu.make_async_remote_copy(
                src_ref=t.at[zi], dst_ref=t.at[zi], send_sem=z_send.at[i], recv_sem=z_recv.at[i],
                device_id=(to, j), device_id_type=MESH,
            )
            for i, t in enumerate((izt, fzt))
        ]

    def yc_copies(k):
        q = lax.rem(yc + k, NY * NC)
        to = (q // NC) * (NZ * NC) + zi * NC + q % NC
        return [
            pltpu.make_async_remote_copy(
                src_ref=t, dst_ref=tab.at[pl.ds(yc * NZ, NZ)], send_sem=meta_send.at[i], recv_sem=meta_recv.at[i],
                device_id=(to, j), device_id_type=MESH,
            )
            for i, (t, tab) in enumerate(((izt, itab), (fzt, ftab)))
        ]

    def all_of(ref, n, send, recv):
        return pltpu.make_async_remote_copy(
            src_ref=ref.at[pl.ds(0, n)], dst_ref=ref.at[pl.ds(0, n)], send_sem=send, recv_sem=recv,
            device_id=(me, (j + 1) % NMP), device_id_type=MESH,
        )

    acts = (act0, act1, act2)
    rcvs = (rcv0, rcv1)

    def hidden(p, act):
        x = pair(p)
        x2 = jnp.concatenate([x, x], axis=0)
        half = hb[p]
        for b in range(F // RB):
            rs = pl.ds(b * RB, RB)
            h = jnp.dot(lw[rs, :], x2, preferred_element_type=F32) * half
            act[rs, :] = (h + h * jnp.tanh(h)).astype(BF)

    def head(p, act):
        vel = jnp.dot(ht[...], act[...], preferred_element_type=F32).astype(BF)
        for q in range(NMP):
            for h in range(2):
                rs = slice(q * Q + h * HQ, q * Q + (h + 1) * HQ)
                xs[h, q, 2 * p] = vel[rs, 0:BT]
                xs[h, q, 2 * p + 1] = vel[rs, BT : 2 * BT]

    with jax.named_scope("forward"):
        hidden(0, act0)
        for p in range(PAIRS):
            if p + 1 < PAIRS:
                hidden(p + 1, acts[(p + 1) % len(acts)])
            head(p, acts[p % len(acts)])
            done = (2 * p + 2) // CS
            if (2 * p + 2) % CS == 0 and done >= OPEN:
                if done == OPEN:
                    pl.semaphore_wait(barrier, NDP - 1 + NMP - 1)
                    for k in range(1, NZ):
                        for c in z_copies(k):
                            c.start()
                for d in (2, 1, 3):
                    xcopy(*SHARES[done - OPEN], d).start()
        for share in SHARES:
            if share[0] == 1:
                for d in (2, 1, 3):
                    xcopy(*share, d).start()

    with jax.named_scope("meta"):
        all_of(izt, NZ - 1, z_send.at[0], z_recv.at[0]).wait_recv()
        all_of(fzt, NZ - 1, z_send.at[1], z_recv.at[1]).wait_recv()
        for k in range(1, NY * NC):
            for c in yc_copies(k):
                c.start()
        itab[pl.ds(yc * NZ, NZ)] = izt[...]
        ftab[pl.ds(yc * NZ, NZ)] = fzt[...]
        c_n.wait()

    def settle(h):
        for share in SHARES:
            if share[0] != h:
                continue
            for d in range(1, NMP):
                xcopy(*share, d).wait_recv()
            for slot in range(share[1] * CS, (share[1] + share[2]) * CS):
                v = xs[h, j, slot].astype(F32) + xr[h, 0, slot].astype(F32)
                v = v + (xr[h, 1, slot].astype(F32) + xr[h, 2, slot].astype(F32))
                predb[h, slot] = v.astype(BF)
                dlt = noi[slot, h * HQ : (h + 1) * HQ, :].astype(F32) + v
                err[h, slot] = dlt * dlt

    def send_blocks(h):
        for o in range(NDP):
            pay[h, o] = predb[h, invs[0, o]]
        for k in SHIFTS:
            p = peer_of(k)
            pltpu.make_async_remote_copy(
                src_ref=pay.at[h, p], dst_ref=rcvs[h].at[me], send_sem=a2a_send.at[h], recv_sem=a2a_recv.at[h],
                device_id=(p, j), device_id_type=MESH,
            ).start()
        rcvs[h][me] = pay[h, me]

    for h in range(2):
        with jax.named_scope("settle%d" % h):
            settle(h)
            if h == 0:
                c_inv.wait()
        with jax.named_scope("send_block%d" % h):
            send_blocks(h)

    et = jnp.zeros((8, 128), F32)
    for s in range(SPD):
        n = (frames[s] - 1) // 32 + 1
        acc = jnp.zeros((HQ, BT), F32)
        for k in range(MAXB):
            acc = acc + jnp.where(k < n, err[0, s * MAXB + k] + err[1, s * MAXB + k], 0.0)
        et = jnp.where(sub == s, jnp.sum(acc, axis=0, keepdims=True), et)
    ext[...] = et
    ex = [
        pltpu.make_async_remote_copy(
            src_ref=ext, dst_ref=exr.at[d - 1], send_sem=ex_send.at[d - 1], recv_sem=ex_recv.at[d - 1],
            device_id=(me, (j + d) % NMP), device_id_type=MESH,
        )
        for d in range(1, NMP)
    ]
    for c in ex:
        c.start()

    with jax.named_scope("tables"):
        all_of(itab, NDP - NZ, meta_send.at[0], meta_recv.at[0]).wait_recv()
        all_of(ftab, NDP - NZ, meta_send.at[1], meta_recv.at[1]).wait_recv()
        c_tab = pltpu.make_async_copy(itab, stab, loc_sem.at[1])
        c_tab.start()

        def prompt(s, carry):
            a, b = carry
            hit = gown == itab[s]
            r = jnp.where(hit & (lane >= NDP), jnp.broadcast_to(ftab[s], (8, 128)), 0.0)
            return a + r, b + r * r

        zero = jnp.zeros((8, 128), F32)
        gsum, gsq = lax.fori_loop(0, NDP, prompt, (zero, zero))
        mean = jnp.sum(gsum, axis=1, keepdims=True) * (1.0 / 12.0)
        var = jnp.sum(gsq, axis=1, keepdims=True) * (1.0 / 12.0) - mean * mean
        adv = (own - mean) / jnp.sqrt(var + 0.25)
        adv_o[...] = jnp.sum(jnp.where(lane == sub, adv, 0.0), axis=0, keepdims=True)
        c_tab.wait()
        idx = jnp.zeros((8, 128), jnp.int32)
        for s in range(NDP):
            src = (s // NZ // NC) * (NZ * NC) + (s % NZ) * NC + (s // NZ) % NC
            idx = jnp.where(lane == stab[s, 0, me], src, idx)
        idxv[...] = idx
        c_idx = pltpu.make_async_copy(idxv, idxs, loc_sem.at[2])
        c_idx.start()
        c_idx.wait()

    def gather_copy(h, d):
        return pltpu.make_async_remote_copy(
            src_ref=rows.at[h], dst_ref=pred_o.at[:, pl.ds(pl.multiple_of(j * Q + h * HQ, HQ), HQ), :],
            send_sem=ag_send.at[h, d - 1], recv_sem=ag_recv.at[h, d - 1],
            device_id=(me, (j + d) % NMP), device_id_type=MESH,
        )

    for h in range(2):
        with jax.named_scope("a2a_wait%d" % h):
            all_of(rcvs[h], NDP - 1, a2a_send.at[h], a2a_recv.at[h]).wait_recv()
        for r in range(OB):
            block = rcvs[h][idxs[0, r]]
            rows[h, r] = block
            pred_o[r, pl.ds(pl.multiple_of(j * Q + h * HQ, HQ), HQ), :] = block
        for d in (2, 1, 3):
            gather_copy(h, d).start()
        if h == 0:
            for c in ex:
                c.wait_recv()
            tot = jnp.sum(ext[...] + exr[0] + (exr[1] + exr[2]), axis=1, keepdims=True)
            lp = -0.5 * tot / (counts * (BT * C)).astype(F32)
            logp_o[...] = jnp.sum(jnp.where(lane == sub, lp, 0.0), axis=0, keepdims=True)

    with jax.named_scope("final_wait"):
        all_of(izt, NZ - 1, z_send.at[0], z_recv.at[0]).wait_send()
        all_of(fzt, NZ - 1, z_send.at[1], z_recv.at[1]).wait_send()
        all_of(itab, NDP - NZ, meta_send.at[0], meta_recv.at[0]).wait_send()
        all_of(ftab, NDP - NZ, meta_send.at[1], meta_recv.at[1]).wait_send()
        for share in SHARES:
            for d in range(1, NMP):
                xcopy(*share, d).wait_send()
        for c in ex:
            c.wait_send()
        for h in range(2):
            all_of(rcvs[h], NDP - 1, a2a_send.at[h], a2a_recv.at[h]).wait_send()
            for d in range(1, NMP):
                gather_copy(h, d).wait()


def local(
    frames, owners, offsets, groups, latent, noise_blocks, rewards, embed_weight, norm_gain, mid_weight, head_weight
):
    hbm = pl.BlockSpec(memory_space=pl.ANY)
    vmem = pl.BlockSpec(memory_space=pltpu.VMEM)
    dma = pltpu.SemaphoreType.DMA
    V = pltpu.VMEM
    S = pltpu.SMEM
    scratch = [
        S((SPD,), jnp.int32), S((SLOTS,), jnp.int32), S((SLOTS,), jnp.int32), S((SPD,), jnp.int32), S((SPD,), F32),
        V((C, D), BF), V((D // 128, 128), F32), V((D, F), BF),
        V((SLOTS, C, BT), BF), V((SLOTS, Q, BT), BF),
        V((2 * C, D), BF), V((F, 2 * C), BF), V((C, F), BF),
        V((SLOTS // 2, 1, 2 * BT), F32), V((F, 2 * BT), BF), V((F, 2 * BT), BF), V((F, 2 * BT), BF),
        V((2, NMP, SLOTS, HQ, BT), BF), V((2, NMP - 1, SLOTS, HQ, BT), BF),
        V((2, SLOTS, HQ, BT), BF), V((2, NDP, HQ, BT), BF), V((NDP, HQ, BT), BF), V((NDP, HQ, BT), BF), V((2, OB, HQ, BT), BF),
        V((NZ, 1, 128), jnp.int32), V((NZ, 1, 128), F32), V((NDP, 1, 128), jnp.int32), V((NDP, 1, 128), F32),
        pltpu.SMEM((NDP, 1, 128), jnp.int32),
        V((8, 128), jnp.int32), pltpu.SMEM((8, 128), jnp.int32),
        V((8, 128), jnp.int32), pltpu.SMEM((8, 128), jnp.int32),
        V((8, 128), F32), V((NMP - 1, 8, 128), F32), V((2, SLOTS, HQ, BT), F32),
        dma((5,)), dma((5,)), dma((MCH,)), dma((3,)),
        dma((2, CHUNKS, NMP - 1)), dma((2, CHUNKS, NMP - 1)),
        dma((2,)), dma((2,)), dma((2,)), dma((2,)), dma((2,)), dma((2,)),
        dma((2, NMP - 1)), dma((2, NMP - 1)), dma((NMP - 1,)), dma((NMP - 1,)),
    ]
    pred, logp, adv = pl.pallas_call(
        kernel,
        out_shape=(
            jax.ShapeDtypeStruct((OB, C, BT), BF),
            jax.ShapeDtypeStruct((1, 128), F32),
            jax.ShapeDtypeStruct((1, 128), F32),
        ),
        in_specs=[hbm] * 11,
        out_specs=(vmem, vmem, vmem),
        scratch_shapes=scratch,
        compiler_params=pltpu.CompilerParams(
            collective_id=0, has_side_effects=True, vmem_limit_bytes=48 * 1024 * 1024
        ),
        name="regroup_forward",
    )(
        *(
            pltpu.with_memory_space_constraint(a, pltpu.HBM)
            for a in (
                frames, owners, offsets, groups, rewards,
                norm_gain.reshape(D // 128, 128), latent, noise_blocks, embed_weight, mid_weight, head_weight.T,
            )
        )
    )
    return pred, logp[0, :SPD], adv[0, :SPD]


def solution(mesh):
    placed = (
        P("dp"), P("dp"), P("dp"), P("dp"), P("dp", None, None), P("dp", None, None), P("dp"),
        P(), P(), P(None, "mp"), P("mp", None),
    )
    return jax.shard_map(
        local,
        mesh=mesh,
        in_specs=placed,
        out_specs=(P("dp", None, None), P("dp"), P("dp")),
        check_vma=False,
    )
```
